256 devices in a mesh: dp: 16 (over z, core), seq: 16 (over x, y).
Axes of the slice: x: 4, y: 4, z: 8, core: 2. Of those that a mesh axis runs over, the one named last changes fastest.
Arguments:
- tokens: bfloat16 [256, 256, 1024], P(('dp', 'seq')), may hold values from -6 to 6
- queries: bfloat16 [256, 256, 1024], P(('dp', 'seq')), may hold values from -240 to 240
- keys: bfloat16 [256, 256, 1024], P(('dp', 'seq')), may hold values from -7 to 7
- values: bfloat16 [256, 256, 1024], P(('dp', 'seq')), may hold values from -6 to 6
- ln_gain: bfloat16 [1024], replicated, may hold values from 0.5 to 1.5
- mean_in: bfloat16 [1024, 2048], P(None, 'seq'), may hold values from -0.1875 to 0.1875
- sigma_in: bfloat16 [1024, 2048], P(None, 'seq'), may hold values from 0.0039978027 to 0.029907227
- noise_in: bfloat16 [1024, 2048], P(None, 'seq'), may hold values from -4 to 4
- mean_out: bfloat16 [2048, 1024], P('seq'), may hold values from -0.125 to 0.125
- sigma_out: bfloat16 [2048, 1024], P('seq'), may hold values from 0.0019989014 to 0.014953613
- noise_out: bfloat16 [2048, 1024], P('seq'), may hold values from -4 to 4
- flip_in: int32 [256, 1024], P('dp'), may hold values from -1 to 1, as said below
- flip_mid: int32 [256, 2048], P('dp', 'seq'), may hold values from -1 to 1, as said below
- flip_hidden: int32 [256, 2048], P('dp', 'seq'), may hold values from -1 to 1, as said below
- flip_out: int32 [256, 1024], P('dp'), may hold values from -1 to 1, as said below
- cotangent: bfloat16 [256, 256, 1024], P(('dp', 'seq')), may hold values from -0.75 to 0.75
Outputs:
- block_out: bfloat16 [256, 256, 1024], P(('dp', 'seq'))
- resid_grad: bfloat16 [256, 256, 1024], P(('dp', 'seq'))
- grad_mean_in: float32 [1024, 2048], P(None, 'seq')
- grad_sigma_in: float32 [1024, 2048], P(None, 'seq')
- grad_mean_out: float32 [2048, 1024], P('seq')
- grad_sigma_out: float32 [2048, 1024], P('seq')
The draws below stay inside these ranges and needn't reach their ends.
Inputs may be any that keep to these rules, and one draw needn't show every extreme that they name: `flip_in`: each entry is -1 or +1. `flip_mid`: each entry is -1 or +1. `flip_hidden`: each entry is -1 or +1. `flip_out`: each entry is -1 or +1.
All inputs are finite; a program needn't handle non-finite values.
Results may differ from the reference program's by a relative error of at most 0.018.
Values may be sent and summed in bfloat16 or wider, within the bound.
A program may use at most 128 MiB of HBM per device.

```python
import math
import jax
import jax.numpy as jnp
from jax import lax

D = 1024
HEADS = 16
FF = 2048
PATCH = 256
IMAGES = 256
N_SEQ = 16


def query_key_pair(key):
    base = jax.random.fold_in(key, 4242)
    key_q, key_k = jax.random.split(base, 2)
    queries = jnp.clip(jax.random.normal(key_q, (IMAGES, PATCH, D), jnp.float32), -6.0, 6.0)
    keys = jnp.clip(jax.random.normal(key_k, (IMAGES, PATCH, D), jnp.float32), -6.0, 6.0)
    return (queries, keys)


def draw_queries(key, part):
    return query_key_pair(key)[0].astype(jnp.bfloat16)


def draw_keys(key, part):
    return query_key_pair(key)[1].astype(jnp.bfloat16)


def sign_table(key, salt, rows, cols):
    bits = jax.random.randint(jax.random.fold_in(key, salt), (rows, cols), 0, 2, jnp.int32)
    return 2 * bits - 1


def draw_flip_in(key, part):
    return sign_table(key, 11, IMAGES, D)


def draw_flip_mid(key, part):
    return sign_table(key, 23, IMAGES, FF)


def draw_flip_hidden(key, part):
    return sign_table(key, 37, IMAGES, FF)


def draw_flip_out(key, part):
    return sign_table(key, 53, IMAGES, D)


def levels(rng, extent, cuts, least, top_value):
    def one(dim, parts):
        heights = jax.random.uniform(jax.random.fold_in(jax.random.fold_in(rng, 6), dim), (parts,), jnp.float32, least / len(cuts), top_value / len(cuts))
        return jnp.repeat(jnp.exp(heights), extent[dim] // parts).reshape((-1,) + (1,) * (len(extent) - dim - 1))

    loudness = one(*cuts[0])
    for cut in cuts[1:]:
        loudness = loudness * one(*cut)
    return loudness


def gaussian(stream_key, extent, width, most, shards=(), kind=jnp.bfloat16):
    result = width * jax.random.normal(stream_key, extent, jnp.float32)
    if shards:
        result = result * levels(stream_key, extent, shards, -0.22, 0.18)
    return jnp.clip(result, -most, most).astype(kind)


def setup_inputs(seed: int = 0) -> dict:
    arg_keys = jax.random.split(jax.random.key(seed), 17)
    return {
        "tokens": gaussian(arg_keys[0], (IMAGES, PATCH, D), 1.0, 6.0, ((0, 256),)),
        "queries": draw_queries(jax.random.fold_in(arg_keys[16], 71), 0),
        "keys": draw_keys(jax.random.fold_in(arg_keys[16], 71), 0),
        "values": gaussian(arg_keys[3], (IMAGES, PATCH, D), 1.0, 6.0, ((0, 256),)),
        "ln_gain": jnp.clip(1.0 + 0.1 * jax.random.normal(arg_keys[4], (D,), jnp.float32), 0.5, 1.5).astype(jnp.bfloat16),
        "mean_in": gaussian(arg_keys[5], (D, FF), D ** -0.5, 0.1875, ((1, 16),)),
        "sigma_in": jnp.clip(jnp.exp(math.log(0.029907227) - 2.01235525 * jax.random.uniform(arg_keys[6], (D, FF), jnp.float32) ** levels(arg_keys[6], (D, FF), ((1, 16),), -0.2, 0.2)), 0.0039978027, 0.029907227).astype(jnp.bfloat16),
        "noise_in": gaussian(arg_keys[7], (D, FF), 1.0, 4.0, ((1, 16),)),
        "mean_out": gaussian(arg_keys[8], (FF, D), FF ** -0.5, 0.125, ((0, 16),)),
        "sigma_out": jnp.clip(jnp.exp(math.log(0.014953613) - 2.01235525 * jax.random.uniform(arg_keys[9], (FF, D), jnp.float32) ** levels(arg_keys[9], (FF, D), ((0, 16),), -0.2, 0.2)), 0.0019989014, 0.014953613).astype(jnp.bfloat16),
        "noise_out": gaussian(arg_keys[10], (FF, D), 1.0, 4.0, ((0, 16),)),
        "flip_in": draw_flip_in(jax.random.fold_in(arg_keys[16], 71), 0),
        "flip_mid": draw_flip_mid(jax.random.fold_in(arg_keys[16], 71), 0),
        "flip_hidden": draw_flip_hidden(jax.random.fold_in(arg_keys[16], 71), 0),
        "flip_out": draw_flip_out(jax.random.fold_in(arg_keys[16], 71), 0),
        "cotangent": gaussian(arg_keys[15], (IMAGES, PATCH, D), 0.125, 0.75, ((0, 256),)),
    }


def attend(query_img, key_img, value_img):
    head_dim = D // HEADS
    qf = query_img.astype(jnp.float32).reshape(PATCH, HEADS, head_dim)
    kf = key_img.astype(jnp.float32).reshape(PATCH, HEADS, head_dim)
    vf = value_img.astype(jnp.float32).reshape(PATCH, HEADS, head_dim)
    scores = jnp.einsum('qhe,khe->hqk', qf, kf) * head_dim ** (-0.5)
    top = lax.optimization_barrier(jnp.max(scores, axis=-1, keepdims=True))
    expd = jnp.exp(scores - top)
    total = lax.optimization_barrier(jnp.sum(expd, axis=-1))
    weights = expd.astype(jnp.bfloat16).astype(jnp.float32)
    outs = jnp.einsum('hqk,khe->qhe', weights, vf) / jnp.transpose(total)[:, :, None]
    return outs.reshape(PATCH, D).astype(jnp.bfloat16)

def gelu_slope(pre):
    cdf = 0.5 * (1.0 + lax.erf(pre * 0.7071067811865476))
    pdf = jnp.exp(-0.5 * pre * pre) * 0.3989422804014327
    return cdf + pre * pdf

def contract_first(left, right):
    return lax.dot_general(left, right, (((0,), (0,)), ((), ())), preferred_element_type=jnp.float32)

def contract_last(left, right):
    return lax.dot_general(left, right, (((1,), (1,)), ((), ())), preferred_element_type=jnp.float32)

def reference(tokens, queries, keys, values, ln_gain, mean_in, sigma_in, noise_in, mean_out, sigma_out, noise_out, flip_in, flip_mid, flip_hidden, flip_out, cotangent):
    bf = jnp.bfloat16
    f32 = jnp.float32
    attn_out = lax.map(lambda trio: attend(trio[0], trio[1], trio[2]), (queries, keys, values))
    resid = (tokens.astype(f32) + attn_out.astype(f32)).astype(bf)
    resid_f = resid.astype(f32)
    centered = resid_f - lax.optimization_barrier(jnp.mean(resid_f, axis=-1, keepdims=True))
    rstd = lax.rsqrt(lax.optimization_barrier(jnp.mean(centered * centered, axis=-1, keepdims=True)) + 1e-06)
    ahat = centered * rstd
    gain_f = ln_gain.astype(f32)
    normed = (ahat * gain_f).astype(bf)
    pert_in = (sigma_in.astype(f32) * noise_in.astype(f32)).astype(bf)
    pert_out = (sigma_out.astype(f32) * noise_out.astype(f32)).astype(bf)
    in_signs = flip_in.astype(bf)[:, None, :]
    mid_signs = flip_mid.astype(f32)[:, None, :]
    hid_signs = flip_hidden.astype(bf)[:, None, :]
    out_signs = flip_out.astype(f32)[:, None, :]
    rows = PATCH * IMAGES
    flat = normed.reshape(rows, D)
    flat_flip = (normed * in_signs).reshape(rows, D)
    pre = jnp.dot(flat, mean_in, preferred_element_type=f32).reshape(IMAGES, PATCH, FF)
    pre = pre + jnp.dot(flat_flip, pert_in, preferred_element_type=f32).reshape(IMAGES, PATCH, FF) * mid_signs
    hidden = jax.nn.gelu(pre, approximate=False).astype(bf)
    flipped_hidden = hidden * hid_signs
    block = FF // N_SEQ
    mixed = jnp.zeros((IMAGES, PATCH, D), f32)
    for index in range(N_SEQ):
        lo = index * block
        hb = hidden[:, :, lo:lo + block].reshape(rows, block)
        hfb = flipped_hidden[:, :, lo:lo + block].reshape(rows, block)
        part = jnp.dot(hb, mean_out[lo:lo + block], preferred_element_type=f32).reshape(IMAGES, PATCH, D)
        part = part + jnp.dot(hfb, pert_out[lo:lo + block], preferred_element_type=f32).reshape(IMAGES, PATCH, D) * out_signs
        mixed = mixed + part.astype(bf).astype(f32)
    block_out = (resid_f + mixed).astype(bf)
    cot_flip = cotangent * flip_out.astype(bf)[:, None, :]
    cot_flat = cotangent.reshape(rows, D)
    cot_flip_flat = cot_flip.reshape(rows, D)
    dhidden = contract_last(cot_flat, mean_out).reshape(IMAGES, PATCH, FF)
    dhidden = dhidden + contract_last(cot_flip_flat, pert_out).reshape(IMAGES, PATCH, FF) * flip_hidden.astype(f32)[:, None, :]
    dpre = (dhidden * gelu_slope(pre)).astype(bf)
    dpre_flip = dpre * flip_mid.astype(bf)[:, None, :]
    grad_mean_out = contract_first(hidden.reshape(rows, FF), cot_flat)
    grad_sigma_out = contract_first(flipped_hidden.reshape(rows, FF), cot_flip_flat) * noise_out.astype(f32)
    grad_mean_in = contract_first(flat, dpre.reshape(rows, FF))
    grad_sigma_in = contract_first(flat_flip, dpre_flip.reshape(rows, FF)) * noise_in.astype(f32)
    dnormed = jnp.zeros((IMAGES, PATCH, D), f32)
    in_signs_f = flip_in.astype(f32)[:, None, :]
    for index in range(N_SEQ):
        lo = index * block
        db = dpre[:, :, lo:lo + block].reshape(rows, block)
        dfb = dpre_flip[:, :, lo:lo + block].reshape(rows, block)
        part = contract_last(db, mean_in[:, lo:lo + block]).reshape(IMAGES, PATCH, D)
        part = part + contract_last(dfb, pert_in[:, lo:lo + block]).reshape(IMAGES, PATCH, D) * in_signs_f
        dnormed = dnormed + part.astype(bf).astype(f32)
    scaled = dnormed * gain_f
    back = rstd * (scaled - lax.optimization_barrier(jnp.mean(scaled, axis=-1, keepdims=True)) - ahat * lax.optimization_barrier(jnp.mean(scaled * ahat, axis=-1, keepdims=True)))
    resid_grad = (cotangent.astype(f32) + back).astype(bf)
    return (block_out, resid_grad, grad_mean_in, grad_sigma_in, grad_mean_out, grad_sigma_out)
```

```python
import functools

import jax
import jax.numpy as jnp
from jax import lax
from jax.experimental import pallas as pl
from jax.experimental.pallas import tpu as pltpu
from jax.sharding import Mesh
from jax.sharding import PartitionSpec as P

BF = jnp.bfloat16
F32 = jnp.float32
HEAD = 64
SIDE = 4
MESH_ID = pl.DeviceIdType.MESH
DP = ("z", "c")
SEQ = ("x", "y")
ALL = ("z", "c", "x", "y")


def dot_t(a, b):
    return lax.dot_general(a, b, (((1,), (1,)), ((), ())), preferred_element_type=F32)


def dot_0(a, b):
    return lax.dot_general(a, b, (((0,), (0,)), ((), ())), preferred_element_type=F32)


def dot_n(a, b):
    return jnp.dot(a, b, preferred_element_type=F32)


class Ring:
    def __init__(self, at, axis, block, sends, recvs, base):
        me = at[axis]
        self.me = me
        self.right = lax.rem(me + 1, SIDE)
        self.left = lax.rem(me + 3, SIDE)
        self.far = lax.rem(me + 2, SIDE)
        self.block = block
        self.sends, self.recvs, self.base = sends, recvs, base

        def device(pos):
            where = dict(at)
            where[axis] = pos
            return tuple(where[name] for name in ALL)

        self.to_right, self.to_left = device(self.right), device(self.left)
        self.live = {}

    def copy(self, slot, src, dst, right):
        return pltpu.make_async_remote_copy(
            src_ref=src,
            dst_ref=dst,
            send_sem=self.sends.at[self.base + slot],
            recv_sem=self.recvs.at[self.base + slot],
            device_id=self.to_right if right else self.to_left,
            device_id_type=MESH_ID,
        )

    def go(self, slot, src, dst, right):
        copy = self.copy(slot, src, dst, right)
        copy.start()
        self.live[slot] = copy

    def gather_start(self):
        for slot, half, right in ((0, 0, True), (1, 1, False), (2, 1, True), (3, 0, False)):
            ref = self.block(self.me, half)
            self.go(slot, ref, ref, right)

    def gather_forward(self):
        self.live[0].wait_recv()
        ref = self.block(self.left, 0)
        self.go(4, ref, ref, True)
        self.live[1].wait_recv()
        ref = self.block(self.right, 1)
        self.go(5, ref, ref, False)

    def gather_finish(self):
        for slot in (2, 3, 4, 5):
            self.live[slot].wait_recv()

    def scatter_start(self, near, once):
        self.near, self.once = near, once
        self.go(0, self.block(self.far, 0), near[0], True)
        self.go(1, self.block(self.far, 1), near[1], False)
        self.go(2, self.block(self.right, 1), once[1], True)
        self.go(3, self.block(self.left, 0), once[2], False)

    def scatter_forward(self, add):
        self.live[0].wait_recv()
        ref = self.block(self.right, 0)
        add(ref, self.near[0])
        self.go(4, ref, self.once[0], True)
        self.live[1].wait_recv()
        ref = self.block(self.left, 1)
        add(ref, self.near[1])
        self.go(5, ref, self.once[3], False)

    def scatter_finish(self, add):
        for slot in (2, 3, 4, 5):
            self.live[slot].wait_recv()
        add(self.block(self.me, 0), self.once[0], self.once[2])
        add(self.block(self.me, 1), self.once[1], self.once[3])

    def drain(self):
        for slot in sorted(self.live):
            self.live[slot].wait_send()


def add_into(ref, *others):
    if len(ref.shape) == 3:
        for i in range(ref.shape[0]):
            add_into(ref.at[i], *(other.at[i] for other in others))
        return
    total = ref[...].astype(F32)
    for other in others:
        total = total + other[...].astype(F32)
    ref[...] = total.astype(BF)


def kernel(
    nz,
    q_ref,
    k_ref,
    v_ref,
    tok_ref,
    cot_ref,
    gain_ref,
    io_ref,
    w_hbm,
    f_hbm,
    out_ref,
    grad_ref,
    sum_ref,
    w_all,
    f_all,
    f_peer,
    io_peer,
    rows,
    norm,
    norm_f,
    cot,
    cot_f,
    resid,
    hid,
    hid_f,
    slope,
    dpre,
    dpre_f,
    mine,
    theirs,
    arrived,
    part,
    near1,
    once1,
    near2,
    once2,
    zbuf,
    total,
    ag_s,
    ag_r,
    rs_s,
    rs_r,
    z_s,
    z_r,
    core_s,
    core_r,
    local,
):
    patches, width = tok_ref.shape
    share = w_hbm.shape[1]
    half = share // 2
    own_hidden = SIDE * SIDE * share
    band = SIDE * share
    nblk = min(256, width)
    at = {name: lax.axis_index(name) for name in ALL}
    z, c, x, y = (at[name] for name in ALL)
    s = x * SIDE + y
    partner = (z, 1 - c, x, y)

    barrier = pltpu.get_barrier_semaphore()
    greet = [
        partner,
        (z, c, lax.rem(x + 1, SIDE), y),
        (z, c, lax.rem(x + 3, SIDE), y),
        (z, c, x, lax.rem(y + 1, SIDE)),
        (z, c, x, lax.rem(y + 3, SIDE)),
    ] + [(lax.rem(z + d, nz), c, x, y) for d in range(1, nz)]
    for device in greet:
        pl.semaphore_signal(barrier, inc=1, device_id=device, device_id_type=MESH_ID)

    loads = [
        pltpu.make_async_copy(w_hbm.at[m], w_all.at[m, x, y], local.at[m]) for m in range(4)
    ] + [pltpu.make_async_copy(f_hbm, f_all.at[x, y], local.at[4])]
    for load in loads:
        load.start()
    for load in loads:
        load.wait()
    pl.semaphore_wait(barrier, len(greet))

    def to_partner(slot, src, dst):
        return pltpu.make_async_remote_copy(
            src_ref=src,
            dst_ref=dst,
            send_sem=core_s.at[slot],
            recv_sem=core_r.at[slot],
            device_id=partner,
            device_id_type=MESH_ID,
        )

    def halves(n):
        return lambda h: pl.ds(h * n, n)

    rows_of = halves(half)
    frows = halves(f_all.shape[2] // 2)

    def gather_rings(m, base):
        if m == 4:
            first = Ring(at, "x", lambda j, h: f_all.at[j, y, frows(h)], ag_s, ag_r, base)
            second = Ring(at, "y", lambda j, h: f_all.at[:, j, frows(h)], ag_s, ag_r, base + 6)
        elif m % 2 == 0:
            first = Ring(at, "x", lambda j, h: w_all.at[m, j, y, rows_of(h)], ag_s, ag_r, base)
            second = Ring(at, "y", lambda j, h: w_all.at[m, :, j, rows_of(h)], ag_s, ag_r, base + 6)
        else:
            first = Ring(at, "y", lambda j, h: w_all.at[m, x, j, rows_of(h)], ag_s, ag_r, base)
            second = Ring(at, "x", lambda j, h: w_all.at[m, j, :, rows_of(h)], ag_s, ag_r, base + 6)
        return first, second

    ag = [gather_rings(m, 12 * m) for m in range(5)]
    order = (4, 0, 1, 2, 3)
    send_cot = to_partner(0, cot_ref, cot.at[pl.ds(patches, patches)])
    send_io = to_partner(1, io_ref, io_peer)
    for m in (4, 0, 1):
        ag[m][0].gather_start()
    send_io.start()
    send_cot.start()
    for m in (2, 3):
        ag[m][0].gather_start()

    def attend(p):
        lanes = pl.ds(pl.multiple_of(p * 128, 128), 128)
        q2, k2, v2 = q_ref[:, lanes], k_ref[:, lanes], v_ref[:, lanes]
        outs = []
        for i in range(2):
            cols = slice(i * HEAD, (i + 1) * HEAD)
            scores = dot_t(q2[:, cols], k2[:, cols]) * (HEAD**-0.5)
            e = jnp.exp(scores - jnp.max(scores, axis=-1, keepdims=True))
            norm_by = jnp.sum(e, axis=-1, keepdims=True)
            outs.append(dot_n(e.astype(BF), v2[:, cols]) / norm_by)
        attn = jnp.concatenate(outs, axis=1).astype(BF)
        resid[:, lanes] = (tok_ref[:, lanes].astype(F32) + attn.astype(F32)).astype(BF)

    pairs = width // 128

    @pl.loop(0, pairs // 2)
    def _(p):
        attend(p)

    for m in order:
        ag[m][0].gather_forward()

    @pl.loop(pairs // 2, pairs)
    def _(p):
        attend(p)

    for m in (4, 0, 1):
        ag[m][0].gather_finish()
        ag[m][1].gather_start()

    chunk = min(64, patches)
    gain = gain_ref[...].astype(F32)

    def stats(r):
        xf = resid[r, :].astype(F32)
        centered = xf - jnp.mean(xf, axis=-1, keepdims=True)
        rstd = lax.rsqrt(jnp.mean(centered * centered, axis=-1, keepdims=True) + 1e-06)
        return xf, centered * rstd, rstd

    @pl.loop(0, patches // chunk)
    def _(i):
        r = pl.ds(pl.multiple_of(i * chunk, chunk), chunk)
        _, ahat, _ = stats(r)
        norm[r, :] = (ahat * gain).astype(BF)
        cot[r, :] = cot_ref[r, :]

    ag[4][1].gather_forward()
    for m in (2, 3):
        ag[m][0].gather_finish()
    ag[4][1].gather_finish()

    send_norm = to_partner(2, norm.at[pl.ds(0, patches)], norm.at[pl.ds(patches, patches)])
    send_norm.start()
    send_flip = to_partner(
        3, f_all.at[:, :, :, pl.ds(2 * share, 2 * share)], f_peer
    )
    send_flip.start()

    send_io.wait_recv()
    send_flip.wait_recv()
    def own_row(t):
        keep = lax.broadcasted_iota(jnp.int32, t.shape, 0) == s
        return jnp.sum(jnp.where(keep, t, 0.0), axis=0, keepdims=True)

    rows[0, 0:2, 0:width] = io_ref[0:2, :]
    rows[1, 0:2, 0:width] = io_peer[0:2, :]
    for i, table in ((0, f_all), (1, f_peer)):
        for a in range(SIDE):
            for b in range(0, SIDE, 2):
                one = own_row(table[a, b, :, 0 : 2 * share])
                two = own_row(table[a, b + 1, :, 0 : 2 * share])
                lanes = slice((a * SIDE + b) * share, (a * SIDE + b + 2) * share)
                rows[i, 2:3, lanes] = jnp.concatenate([one[:, :share], two[:, :share]], axis=1)
                rows[i, 3:4, lanes] = jnp.concatenate([one[:, share:], two[:, share:]], axis=1)

    send_cot.wait_recv()
    send_norm.wait_recv()

    @pl.loop(0, patches // chunk)
    def _(i):
        for image in range(2):
            r = pl.ds(pl.multiple_of(image * patches + i * chunk, chunk), chunk)
            norm_f[r, :] = norm[r, :] * rows[image, 0:1, 0:width].astype(BF)
            cot_f[r, :] = cot[r, :] * rows[image, 1:2, 0:width].astype(BF)

    for m in (0, 1):
        ag[m][1].gather_forward()
    for m in (2, 3):
        ag[m][1].gather_start()
    for m in (0, 1):
        ag[m][1].gather_finish()

    image_rows = [slice(i * patches, (i + 1) * patches) for i in range(2)]

    def weight(m, h):
        return w_all[m, h].reshape(band, width)

    def weight_grad(m, h, left, right):
        for n in range(width // nblk):
            cols = slice(n * nblk, (n + 1) * nblk)
            part[m, h, :, :, cols] = (
                dot_0(left, right[:, cols]).astype(BF).reshape(SIDE, share, nblk)
            )

    def forward(h):
        lanes = pl.ds(pl.multiple_of(h * band, band), band)
        for i, r in enumerate(image_rows):
            pre = dot_t(norm[r, :], weight(0, h))
            pre = pre + dot_t(norm_f[r, :], weight(1, h)) * rows[i, 2:3, lanes]
            cdf = 0.5 * (1.0 + lax.erf(pre * 0.7071067811865476))
            pdf = jnp.exp(-0.5 * pre * pre) * 0.3989422804014327
            slope[r, lanes] = cdf + pre * pdf
            unit = (pre * cdf).astype(BF)
            hid[r, lanes] = unit
            hid_f[r, lanes] = unit * rows[i, 3:4, lanes].astype(BF)
        weight_grad(2, h, hid[:, lanes], cot)
        weight_grad(3, h, hid_f[:, lanes], cot_f)

    def backward(h):
        lanes = pl.ds(pl.multiple_of(h * band, band), band)
        for i, r in enumerate(image_rows):
            dh = dot_t(cot[r, :], weight(2, h))
            dh = dh + dot_t(cot_f[r, :], weight(3, h)) * rows[i, 3:4, lanes]
            unit = (dh * slope[r, lanes]).astype(BF)
            dpre[r, lanes] = unit
            dpre_f[r, lanes] = unit * rows[i, 2:3, lanes].astype(BF)
        weight_grad(0, h, dpre[:, lanes], norm)
        weight_grad(1, h, dpre_f[:, lanes], norm_f)

    def scatter_rings(m, base):
        along_y = lambda j, h: part.at[m, :, j, rows_of(h)]
        along_x = lambda j, h: part.at[m, j, :, rows_of(h)]
        one = lambda j, h: part.at[m, j, y, rows_of(h)]
        two = lambda j, h: part.at[m, x, j, rows_of(h)]
        if m % 2 == 0:
            return Ring(at, "y", along_y, rs_s, rs_r, base), Ring(at, "x", one, rs_s, rs_r, base + 6)
        return Ring(at, "x", along_x, rs_s, rs_r, base), Ring(at, "y", two, rs_s, rs_r, base + 6)

    rs = [scatter_rings(m, 12 * m) for m in range(4)]

    def start1(m):
        rs[m][0].scatter_start([near1.at[m, k] for k in range(2)], [once1.at[m, k] for k in range(4)])

    def start2(m):
        rs[m][1].scatter_start([near2.at[m, k] for k in range(2)], [once2.at[m, k] for k in range(4)])

    row_groups = min(nz, 4)
    lane_groups = nz // row_groups
    zr, zl = share // row_groups, width // lane_groups

    def spot(j):
        return (
            pl.ds(pl.multiple_of(lax.div(j, lane_groups) * zr, zr), zr),
            pl.ds(pl.multiple_of(lax.rem(j, lane_groups) * zl, zl), zl),
        )

    z_live = {}

    def z_copy(m, d, stage, src, dst):
        copy = pltpu.make_async_remote_copy(
            src_ref=src,
            dst_ref=dst,
            send_sem=z_s.at[m, stage, d - 1],
            recv_sem=z_r.at[m, stage, d - 1],
            device_id=(lax.rem(z + d, nz), c, x, y),
            device_id_type=MESH_ID,
        )
        copy.start()
        z_live[m, stage, d] = copy

    def z_start(m):
        for d in range(1, nz):
            r, l = spot(lax.rem(z + d, nz))
            z_copy(m, d, 0, part.at[m, x, y, r, l], zbuf.at[m, d - 1])

    def z_spread(m):
        r, l = spot(z)
        acc = part[m, x, y, r, l].astype(F32)
        for d in range(1, nz):
            z_live[m, 0, d].wait_recv()
            acc = acc + zbuf[m, d - 1].astype(F32)
        total[m, c, r, l] = acc.astype(BF)
        for d in range(1, nz):
            place = total.at[m, c, r, l]
            z_copy(m, d, 1, place, place)

    z_last = {}

    def z_finish(m):
        for d in range(1, nz):
            z_live[m, 1, d].wait_recv()
        z_last[m] = to_partner(6 + m, total.at[m, c], total.at[m, c])
        z_last[m].start()

    bands = own_hidden // band

    @pl.loop(0, bands // 2)
    def _(h):
        forward(h)

    for m in (2, 3):
        ag[m][1].gather_forward()

    @pl.loop(bands // 2, bands)
    def _(h):
        forward(h)

    start1(2)
    start1(3)
    for m in (2, 3):
        ag[m][1].gather_finish()

    @pl.loop(0, bands // 2)
    def _(h):
        backward(h)

    for m in (2, 3):
        rs[m][0].scatter_forward(add_into)

    @pl.loop(bands // 2, bands)
    def _(h):
        backward(h)

    start1(0)
    start1(1)

    def project(left, left_f, m, sign):
        @pl.loop(0, width // nblk)
        def _(n):
            lanes = pl.ds(pl.multiple_of(n * nblk, nblk), nblk)
            plain = w_all[m, :, :, :, lanes].reshape(own_hidden, nblk)
            noisy = w_all[m + 1, :, :, :, lanes].reshape(own_hidden, nblk)
            for i, r in enumerate(image_rows):
                out = dot_n(left[r, :], plain)
                out = out + dot_n(left_f[r, :], noisy) * rows[i, sign : sign + 1, lanes]
                if i:
                    theirs[m // 2, :, lanes] = out.astype(BF)
                else:
                    mine[m // 2, :, lanes] = out

    project(hid, hid_f, 2, 1)
    send_mixed = to_partner(4, theirs.at[1], arrived.at[1])
    send_mixed.start()

    for m in (2, 3):
        rs[m][0].scatter_finish(add_into)
        start2(m)

    project(dpre, dpre_f, 0, 0)
    send_back = to_partner(5, theirs.at[0], arrived.at[0])
    send_back.start()

    for m in (2, 3):
        rs[m][1].scatter_forward(add_into)
    for m in (0, 1):
        rs[m][0].scatter_forward(add_into)

    send_mixed.wait_recv()
    send_back.wait_recv()

    @pl.loop(0, patches // chunk)
    def _(i):
        r = pl.ds(pl.multiple_of(i * chunk, chunk), chunk)
        xf, ahat, rstd = stats(r)
        out_ref[r, :] = (xf + mine[1, r, :] + arrived[1, r, :].astype(F32)).astype(BF)
        g = (mine[0, r, :] + arrived[0, r, :].astype(F32)) * gain
        back = rstd * (
            g
            - jnp.mean(g, axis=-1, keepdims=True)
            - ahat * jnp.mean(g * ahat, axis=-1, keepdims=True)
        )
        grad_ref[r, :] = (cot_ref[r, :].astype(F32) + back).astype(BF)

    for m in (2, 3):
        rs[m][1].scatter_finish(add_into)
        z_start(m)
    for m in (0, 1):
        rs[m][0].scatter_finish(add_into)
        start2(m)
    for m in (2, 3):
        z_spread(m)
    for m in (0, 1):
        rs[m][1].scatter_forward(add_into)
    for m in (2, 3):
        z_finish(m)
    for m in (0, 1):
        rs[m][1].scatter_finish(add_into)
        z_start(m)
    for m in (0, 1):
        z_spread(m)
    for m in (0, 1):
        z_finish(m)
    for m in (2, 3, 0, 1):
        z_last[m].wait_recv()
    sum_ref[...] = total[...]

    for first, second in ag + rs:
        first.drain()
        second.drain()
    for copy in z_live.values():
        copy.wait_send()
    for copy in [send_cot, send_io, send_norm, send_flip, send_mixed, send_back, *z_last.values()]:
        copy.wait_send()


def layer(q, k, v, tok, cot, gain, io, w, f, nz):
    patches, width = tok.shape
    share = w.shape[1]
    hidden = SIDE * SIDE * share
    both = 2 * patches
    row_groups = min(nz, 4)
    zr, zl = share // row_groups, width // (nz // row_groups)
    vmem = pl.BlockSpec(memory_space=pltpu.VMEM)
    any_space = pl.BlockSpec(memory_space=pl.ANY)
    dma = pltpu.SemaphoreType.DMA
    half = share // 2
    scratch = [
        pltpu.VMEM((4, SIDE, SIDE, share, width), BF),
        pltpu.VMEM((SIDE, SIDE, *f.shape), F32),
        pltpu.VMEM((SIDE, SIDE, f.shape[0], f.shape[1] // 2), F32),
        pltpu.VMEM(io.shape, F32),
        pltpu.VMEM((2, 8, max(width, hidden)), F32),
        pltpu.VMEM((both, width), BF),
        pltpu.VMEM((both, width), BF),
        pltpu.VMEM((both, width), BF),
        pltpu.VMEM((both, width), BF),
        pltpu.VMEM((patches, width), BF),
        pltpu.VMEM((both, hidden), BF),
        pltpu.VMEM((both, hidden), BF),
        pltpu.VMEM((both, hidden), F32),
        pltpu.VMEM((both, hidden), BF),
        pltpu.VMEM((both, hidden), BF),
        pltpu.VMEM((2, patches, width), F32),
        pltpu.VMEM((2, patches, width), BF),
        pltpu.VMEM((2, patches, width), BF),
        pltpu.VMEM((4, SIDE, SIDE, share, width), BF),
        pltpu.VMEM((4, 2, SIDE, half, width), BF),
        pltpu.VMEM((4, 4, SIDE, half, width), BF),
        pltpu.VMEM((4, 2, half, width), BF),
        pltpu.VMEM((4, 4, half, width), BF),
        pltpu.VMEM((4, nz - 1, zr, zl), BF),
        pltpu.VMEM((4, 2, share, width), BF),
        dma((60,)),
        dma((60,)),
        dma((48,)),
        dma((48,)),
        dma((4, 2, nz - 1)),
        dma((4, 2, nz - 1)),
        dma((10,)),
        dma((10,)),
        dma((5,)),
    ]
    return pl.pallas_call(
        functools.partial(kernel, nz),
        out_shape=(
            jax.ShapeDtypeStruct((patches, width), BF),
            jax.ShapeDtypeStruct((patches, width), BF),
            jax.ShapeDtypeStruct((4, 2, share, width), BF),
        ),
        in_specs=[vmem] * 7 + [any_space] * 2,
        out_specs=(vmem, vmem, vmem),
        scratch_shapes=scratch,
        compiler_params=pltpu.CompilerParams(
            collective_id=0, has_side_effects=True, vmem_limit_bytes=62 * 1024 * 1024
        ),
        name="layer",
    )(q, k, v, tok, cot, gain, io, w, f)


def body(
    tokens,
    queries,
    keys,
    values,
    ln_gain,
    mean_in,
    sigma_in,
    noise_in,
    mean_out,
    sigma_out,
    noise_out,
    flip_in,
    flip_mid,
    flip_hidden,
    flip_out,
    cotangent,
):
    nz = lax.axis_size("z")
    width = tokens.shape[-1]
    share = mean_in.shape[1] // 2
    c = lax.axis_index("c")
    s = lax.axis_index("x") * SIDE + lax.axis_index("y")
    pert_in = (sigma_in.astype(F32) * noise_in.astype(F32)).astype(BF)
    pert_out = (sigma_out.astype(F32) * noise_out.astype(F32)).astype(BF)

    def own(t, axis):
        return lax.dynamic_slice_in_dim(t, c * share, share, axis)

    w = jnp.stack([own(mean_in, 1).T, own(pert_in, 1).T, own(mean_out, 0), own(pert_out, 0)])
    mid, hidden = flip_mid.astype(F32), flip_hidden.astype(F32)
    pick = lambda t, first: jnp.where((c == 0) == first, t[:, :share], t[:, share:])
    f = jnp.concatenate(
        [pick(mid, True), pick(hidden, True), pick(mid, False), pick(hidden, False)], axis=1
    )
    io = jnp.stack(
        [lax.dynamic_index_in_dim(t, s, 0, False).astype(F32) for t in (flip_in, flip_out)]
    )
    io = jnp.pad(io, ((0, 6), (0, 0)))
    out, grad, sums = layer(
        queries[0], keys[0], values[0], tokens[0], cotangent[0], ln_gain.reshape(1, width), io, w, f, nz
    )
    sums = sums.astype(F32).reshape(4, 2 * share, width)
    grad_mean_in = sums[0].T
    grad_sigma_in = sums[1].T * noise_in.astype(F32)
    grad_mean_out = sums[2]
    grad_sigma_out = sums[3] * noise_out.astype(F32)
    return out[None], grad[None], grad_mean_in, grad_sigma_in, grad_mean_out, grad_sigma_out


def solution(mesh):
    finer = Mesh(mesh.devices.reshape(-1, 2, SIDE, SIDE), ALL)
    images = P(ALL, None, None)
    cols = P(None, SEQ)
    rows = P(SEQ, None)
    in_specs = (
        images,
        images,
        images,
        images,
        P(),
        cols,
        cols,
        cols,
        rows,
        rows,
        rows,
        P(DP, None),
        P(DP, SEQ),
        P(DP, SEQ),
        P(DP, None),
        images,
    )
    out_specs = (images, images, cols, cols, rows, rows)
    return jax.shard_map(body, mesh=finer, in_specs=in_specs, out_specs=out_specs, check_vma=False)
```

```python
import functools

import jax
import jax.numpy as jnp
from jax import lax
from jax.experimental import pallas as pl
from jax.experimental.pallas import tpu as pltpu
from jax.sharding import Mesh
from jax.sharding import PartitionSpec as P

BF = jnp.bfloat16
F32 = jnp.float32
HEAD = 64
SIDE = 4
MESH_ID = pl.DeviceIdType.MESH
DP = ("z", "c")
SEQ = ("x", "y")
ALL = ("z", "c", "x", "y")


def dot_t(a, b):
    return lax.dot_general(a, b, (((1,), (1,)), ((), ())), preferred_element_type=F32)


def dot_0(a, b):
    return lax.dot_general(a, b, (((0,), (0,)), ((), ())), preferred_element_type=F32)


def dot_n(a, b):
    return jnp.dot(a, b, preferred_element_type=F32)


class Ring:
    def __init__(self, at, axis, block, sends, recvs, base):
        me = at[axis]
        self.me = me
        self.right = lax.rem(me + 1, SIDE)
        self.left = lax.rem(me + 3, SIDE)
        self.far = lax.rem(me + 2, SIDE)
        self.block = block
        self.sends, self.recvs, self.base = sends, recvs, base

        def device(pos):
            where = dict(at)
            where[axis] = pos
            return tuple(where[name] for name in ALL)

        self.to_right, self.to_left = device(self.right), device(self.left)
        self.live = {}

    def copy(self, slot, src, dst, right):
        return pltpu.make_async_remote_copy(
            src_ref=src,
            dst_ref=dst,
            send_sem=self.sends.at[self.base + slot],
            recv_sem=self.recvs.at[self.base + slot],
            device_id=self.to_right if right else self.to_left,
            device_id_type=MESH_ID,
        )

    def go(self, slot, src, dst, right):
        copy = self.copy(slot, src, dst, right)
        copy.start()
        self.live[slot] = copy

    def gather_start(self):
        for slot, half, right in ((0, 0, True), (1, 1, False), (2, 1, True), (3, 0, False)):
            ref = self.block(self.me, half)
            self.go(slot, ref, ref, right)

    def gather_forward(self):
        self.live[0].wait_recv()
        ref = self.block(self.left, 0)
        self.go(4, ref, ref, True)
        self.live[1].wait_recv()
        ref = self.block(self.right, 1)
        self.go(5, ref, ref, False)

    def gather_finish(self):
        for slot in (2, 3, 4, 5):
            self.live[slot].wait_recv()

    def scatter_start(self, near, once):
        self.near, self.once = near, once
        self.go(0, self.block(self.far, 0), near[0], True)
        self.go(1, self.block(self.far, 1), near[1], False)
        self.go(2, self.block(self.right, 1), once[1], True)
        self.go(3, self.block(self.left, 0), once[2], False)

    def scatter_forward(self, add):
        self.live[0].wait_recv()
        ref = self.block(self.right, 0)
        add(ref, self.near[0])
        self.go(4, ref, self.once[0], True)
        self.live[1].wait_recv()
        ref = self.block(self.left, 1)
        add(ref, self.near[1])
        self.go(5, ref, self.once[3], False)

    def scatter_finish(self, add):
        for slot in (2, 3, 4, 5):
            self.live[slot].wait_recv()
        add(self.block(self.me, 0), self.once[0], self.once[2])
        add(self.block(self.me, 1), self.once[1], self.once[3])

    def drain(self):
        for slot in sorted(self.live):
            self.live[slot].wait_send()


def add_into(ref, *others):
    if len(ref.shape) == 3:
        for i in range(ref.shape[0]):
            add_into(ref.at[i], *(other.at[i] for other in others))
        return
    total = ref[...].astype(F32)
    for other in others:
        total = total + other[...].astype(F32)
    ref[...] = total.astype(BF)


def kernel(
    nz,
    q_ref,
    k_ref,
    v_ref,
    tok_ref,
    cot_ref,
    gain_ref,
    io_ref,
    w_hbm,
    f_hbm,
    out_ref,
    grad_ref,
    sum_ref,
    w_all,
    f_all,
    msg,
    signs,
    norm,
    norm_f,
    cot,
    cot_f,
    resid,
    hid,
    hid_f,
    slope,
    dpre,
    dpre_f,
    mine,
    theirs,
    arrived,
    part,
    near1,
    once1,
    near2,
    once2,
    zbuf,
    total,
    ag_s,
    ag_r,
    rs_s,
    rs_r,
    z_s,
    z_r,
    core_s,
    core_r,
    local,
):
    patches, width = tok_ref.shape
    share = w_hbm.shape[1]
    half = share // 2
    own_hidden = SIDE * SIDE * share
    band = min(256, own_hidden)
    per_band = band // (SIDE * share)
    bands = own_hidden // band
    nblk = min(256, width)
    nk = nz // 2
    at = {name: lax.axis_index(name) for name in ALL}
    z, c, x, y = (at[name] for name in ALL)
    s = x * SIDE + y
    zp, zk = lax.rem(z, 2), lax.div(z, 2)
    other = z + 1 - 2 * zp
    partner, mate, cross = (z, 1 - c, x, y), (other, c, x, y), (other, 1 - c, x, y)

    barrier = pltpu.get_barrier_semaphore()
    greet = [
        partner,
        cross,
        (z, c, lax.rem(x + 1, SIDE), y),
        (z, c, lax.rem(x + 3, SIDE), y),
        (z, c, x, lax.rem(y + 1, SIDE)),
        (z, c, x, lax.rem(y + 3, SIDE)),
    ] + [(lax.rem(z + d, nz), c, x, y) for d in range(1, nz)]
    for device in greet:
        pl.semaphore_signal(barrier, inc=1, device_id=device, device_id_type=MESH_ID)

    loads = [
        pltpu.make_async_copy(w_hbm.at[m], w_all.at[m, x, y], local.at[m]) for m in range(4)
    ] + [pltpu.make_async_copy(f_hbm, f_all.at[x, y], local.at[4])]
    for load in loads:
        load.start()
    for load in loads:
        load.wait()
    pl.semaphore_wait(barrier, len(greet))

    def remote(slot, src, dst, device):
        return pltpu.make_async_remote_copy(
            src_ref=src,
            dst_ref=dst,
            send_sem=core_s.at[slot],
            recv_sem=core_r.at[slot],
            device_id=device,
            device_id_type=MESH_ID,
        )

    def halves(n):
        return lambda h: pl.ds(h * n, n)

    rows_of = halves(half)
    frows = halves(f_all.shape[2] // 2)

    def gather_rings(m, base):
        if m == 4:
            first = Ring(at, "x", lambda j, h: f_all.at[j, y, frows(h)], ag_s, ag_r, base)
            second = Ring(at, "y", lambda j, h: f_all.at[:, j, frows(h)], ag_s, ag_r, base + 6)
        elif m % 2 == 0:
            first = Ring(at, "x", lambda j, h: w_all.at[m, j, y, rows_of(h)], ag_s, ag_r, base)
            second = Ring(at, "y", lambda j, h: w_all.at[m, :, j, rows_of(h)], ag_s, ag_r, base + 6)
        else:
            first = Ring(at, "y", lambda j, h: w_all.at[m, x, j, rows_of(h)], ag_s, ag_r, base)
            second = Ring(at, "x", lambda j, h: w_all.at[m, j, :, rows_of(h)], ag_s, ag_r, base + 6)
        return first, second

    def slot_rows(i):
        return pl.ds(i * patches, patches)

    ag = [gather_rings(m, 12 * m) for m in range(5)]
    sends = []

    def send(slot, src, dst, device):
        copy = remote(slot, src, dst, device)
        copy.start()
        sends.append(copy)
        return copy

    for m in (4, 0, 1):
        ag[m][0].gather_start()
    cot_1 = send(0, cot_ref, cot.at[slot_rows(1)], partner)
    cot_2 = send(1, cot_ref, cot.at[slot_rows(2)], mate)
    for m in (2, 3):
        ag[m][0].gather_start()

    def attend(p):
        lanes = pl.ds(pl.multiple_of(p * 128, 128), 128)
        q2, k2, v2 = q_ref[:, lanes], k_ref[:, lanes], v_ref[:, lanes]
        outs = []
        for i in range(2):
            cols = slice(i * HEAD, (i + 1) * HEAD)
            scores = dot_t(q2[:, cols], k2[:, cols]) * (HEAD**-0.5)
            e = jnp.exp(scores - jnp.max(scores, axis=-1, keepdims=True))
            norm_by = jnp.sum(e, axis=-1, keepdims=True)
            outs.append(dot_n(e.astype(BF), v2[:, cols]) / norm_by)
        attn = jnp.concatenate(outs, axis=1).astype(BF)
        resid[:, lanes] = (tok_ref[:, lanes].astype(F32) + attn.astype(F32)).astype(BF)

    pairs = width // 128

    @pl.loop(0, pairs // 2)
    def _(p):
        attend(p)

    for m in (4, 0, 1, 2, 3):
        ag[m][0].gather_forward()

    @pl.loop(pairs // 2, pairs)
    def _(p):
        attend(p)

    for m in (4, 0, 1):
        ag[m][0].gather_finish()
        ag[m][1].gather_start()

    chunk = min(64, patches)
    gain = gain_ref[...].astype(F32)

    def stats(r):
        xf = resid[r, :].astype(F32)
        centered = xf - jnp.mean(xf, axis=-1, keepdims=True)
        rstd = lax.rsqrt(jnp.mean(centered * centered, axis=-1, keepdims=True) + 1e-06)
        return xf, centered * rstd, rstd

    @pl.loop(0, patches // chunk)
    def _(i):
        r = pl.ds(pl.multiple_of(i * chunk, chunk), chunk)
        _, ahat, _ = stats(r)
        norm[r, :] = (ahat * gain).astype(BF)
        cot[r, :] = cot_ref[r, :]

    for m in (2, 3):
        ag[m][0].gather_finish()
        ag[m][1].gather_start()
    norm_1 = send(3, norm.at[slot_rows(0)], norm.at[slot_rows(1)], partner)
    norm_2 = send(4, norm.at[slot_rows(0)], norm.at[slot_rows(2)], mate)
    ag[4][1].gather_forward()
    ag[4][1].gather_finish()

    def own_row(t):
        keep = lax.broadcasted_iota(jnp.int32, t.shape, 0) == s
        return jnp.sum(jnp.where(keep, t, 0.0), axis=0, keepdims=True)

    for t in range(4):
        msg[t, 0:2, 0:width] = io_ref[0:2, :]
    for a in range(SIDE):
        picked = [own_row(f_all[a, b]) for b in range(SIDE)]
        for t in range(4):
            for kind in range(2):
                lo = (kind * 4 + t) * share
                first = kind * own_hidden + a * SIDE * share
                msg[t, 2:3, first : first + SIDE * share] = jnp.concatenate(
                    [row[:, lo : lo + share] for row in picked], axis=1
                )
    quarter = lambda core, parity: msg.at[2 * core + parity]
    sign_1 = send(6, quarter(1 - c, zp), signs.at[1], partner)
    sign_2 = send(7, quarter(c, 1 - zp), signs.at[2], mate)
    sign_3 = send(8, quarter(1 - c, 1 - zp), signs.at[3], cross)
    signs[0] = msg[2 * c + zp]

    def flip(dst, src, slot, row):
        @pl.loop(0, patches // chunk)
        def _(i):
            r = pl.ds(pl.multiple_of(slot * patches + i * chunk, chunk), chunk)
            dst[r, :] = src[r, :] * signs[slot, row : row + 1, 0:width].astype(BF)

    for m in (0, 1):
        ag[m][1].gather_forward()
    flip(norm_f, norm, 0, 0)
    flip(cot_f, cot, 0, 1)
    for copy in (cot_1, norm_1, sign_1):
        copy.wait_recv()
    flip(norm_f, norm, 1, 0)
    flip(cot_f, cot, 1, 1)
    for m in (2, 3):
        ag[m][1].gather_forward()
    cot_2.wait_recv()
    cot_3 = send(2, cot.at[slot_rows(2)], cot.at[slot_rows(3)], partner)
    for m in (0, 1):
        ag[m][1].gather_finish()

    def weight(m, h):
        return w_all[m, pl.ds(h * per_band, per_band)].reshape(band, width)

    def spans(t):
        i, h = lax.div(t, bands), lax.rem(t, bands)
        return (
            i,
            h,
            pl.ds(pl.multiple_of(i * patches, patches), patches),
            pl.ds(pl.multiple_of(h * band, band), band),
        )

    def hidden_row(i, h):
        return signs[i, 2:3, pl.ds(pl.multiple_of(own_hidden + h * band, band), band)]

    def forward(first, last):
        @pl.loop(first * bands, last * bands)
        def _(t):
            i, h, r, lanes = spans(t)
            pre = dot_t(norm[r, :], weight(0, h))
            pre = pre + dot_t(norm_f[r, :], weight(1, h)) * signs[i, 2:3, lanes]
            cdf = 0.5 * (1.0 + lax.erf(pre * 0.7071067811865476))
            pdf = jnp.exp(-0.5 * pre * pre) * 0.3989422804014327
            slope[r, lanes] = cdf + pre * pdf
            unit = (pre * cdf).astype(BF)
            hid[r, lanes] = unit
            hid_f[r, lanes] = unit * hidden_row(i, h).astype(BF)

    def backward(first, last):
        @pl.loop(first * bands, last * bands)
        def _(t):
            i, h, r, lanes = spans(t)
            dh = dot_t(cot[r, :], weight(2, h))
            dh = dh + dot_t(cot_f[r, :], weight(3, h)) * hidden_row(i, h)
            unit = (dh * slope[r, lanes]).astype(BF)
            dpre[r, lanes] = unit
            dpre_f[r, lanes] = unit * signs[i, 2:3, lanes].astype(BF)

    def weight_grad(m, left, right):
        @pl.loop(0, bands)
        def _(h):
            lhs = left[:, pl.ds(pl.multiple_of(h * band, band), band)]
            for n in range(width // nblk):
                cols = slice(n * nblk, (n + 1) * nblk)
                part[m, pl.ds(h * per_band, per_band), :, :, cols] = (
                    dot_0(lhs, right[:, cols]).astype(BF).reshape(per_band, SIDE, share, nblk)
                )

    def scatter_rings(m, base):
        along_y = lambda j, h: part.at[m, :, j, rows_of(h)]
        along_x = lambda j, h: part.at[m, j, :, rows_of(h)]
        one = lambda j, h: part.at[m, j, y, rows_of(h)]
        two = lambda j, h: part.at[m, x, j, rows_of(h)]
        if m % 2 == 0:
            return Ring(at, "y", along_y, rs_s, rs_r, base), Ring(at, "x", one, rs_s, rs_r, base + 6)
        return Ring(at, "x", along_x, rs_s, rs_r, base), Ring(at, "y", two, rs_s, rs_r, base + 6)

    rs = [scatter_rings(m, 12 * m) for m in range(4)]

    def start1(m):
        rs[m][0].scatter_start([near1.at[m, k] for k in range(2)], [once1.at[m, k] for k in range(4)])

    def start2(m):
        rs[m][1].scatter_start([near2.at[m, k] for k in range(2)], [once2.at[m, k] for k in range(4)])

    row_groups = min(nk, 2)
    lane_groups = nk // row_groups
    zr, zl = share // row_groups, width // lane_groups

    def spot(j):
        return (
            pl.ds(pl.multiple_of(lax.div(j, lane_groups) * zr, zr), zr),
            pl.ds(pl.multiple_of(lax.rem(j, lane_groups) * zl, zl), zl),
        )

    z_live = {}

    def z_copy(m, stage, d, step, src, dst):
        copy = pltpu.make_async_remote_copy(
            src_ref=src,
            dst_ref=dst,
            send_sem=z_s.at[m, stage, d - 1],
            recv_sem=z_r.at[m, stage, d - 1],
            device_id=(lax.rem(z + step * d, nz), c, x, y),
            device_id_type=MESH_ID,
        )
        copy.start()
        z_live[m, stage, d] = copy

    def z_start(m):
        for d in range(1, nk):
            r, l = spot(lax.rem(zk + d, nk))
            z_copy(m, 0, d, 2, part.at[m, x, y, r, l], zbuf.at[m, d - 1])

    def z_spread(m):
        r, l = spot(zk)
        acc = part[m, x, y, r, l].astype(F32)
        for d in range(1, nk):
            z_live[m, 0, d].wait_recv()
            acc = acc + zbuf[m, d - 1].astype(F32)
        total[m, c, zp, r, l] = acc.astype(BF)
        for d in range(1, nz):
            place = total.at[m, c, zp, r, l]
            z_copy(m, 1, d, 1, place, place)

    z_last = {}

    def z_finish(m):
        for d in range(1, nz):
            z_live[m, 1, d].wait_recv()
        z_last[m] = send(15 + m, total.at[m, c], total.at[m, c], partner)

    def project(left, left_f, t, sign):
        m = 2 * t

        @pl.loop(0, width // nblk)
        def _(n):
            lanes = pl.ds(pl.multiple_of(n * nblk, nblk), nblk)
            plain = w_all[m, :, :, :, lanes].reshape(own_hidden, nblk)
            noisy = w_all[m + 1, :, :, :, lanes].reshape(own_hidden, nblk)
            for i in range(4):
                r = slice(i * patches, (i + 1) * patches)
                out = dot_n(left[r, :], plain)
                out = out + dot_n(left_f[r, :], noisy) * signs[i, sign : sign + 1, lanes]
                if i:
                    theirs[t, i - 1, :, lanes] = out.astype(BF)
                else:
                    mine[t, :, lanes] = out

        base = 12 - 3 * t
        to_pair = send(base, theirs.at[t, 0], arrived.at[t, 0], partner)
        to_far = send(base + 1, theirs.at[t, 2], arrived.at[t, 1], partner)
        return to_pair, to_far

    def relay(t, to_far):
        to_far.wait_recv()

        @pl.loop(0, patches // chunk)
        def _(i):
            r = pl.ds(pl.multiple_of(i * chunk, chunk), chunk)
            both = theirs[t, 1, r, :].astype(F32) + arrived[t, 1, r, :].astype(F32)
            theirs[t, 1, r, :] = both.astype(BF)

        return send(14 - 3 * t, theirs.at[t, 1], arrived.at[t, 2], mate)

    forward(0, 2)
    sign_2.wait_recv()
    flip(cot_f, cot, 2, 1)
    norm_2.wait_recv()
    norm_3 = send(5, norm.at[slot_rows(2)], norm.at[slot_rows(3)], partner)
    flip(norm_f, norm, 2, 0)
    forward(2, 3)
    sign_3.wait_recv()
    cot_3.wait_recv()
    flip(cot_f, cot, 3, 1)
    norm_3.wait_recv()
    flip(norm_f, norm, 3, 0)
    forward(3, 4)
    weight_grad(2, hid, cot)
    start1(2)
    weight_grad(3, hid_f, cot_f)
    start1(3)
    for m in (2, 3):
        ag[m][1].gather_finish()
    mixed_1, mixed_far = project(hid, hid_f, 1, 1)
    backward(0, 4)
    mixed_2 = relay(1, mixed_far)
    for m in (2, 3):
        rs[m][0].scatter_forward(add_into)
    weight_grad(0, dpre, norm)
    start1(0)
    weight_grad(1, dpre_f, norm_f)
    start1(1)
    for m in (2, 3):
        rs[m][0].scatter_finish(add_into)
        start2(m)
    back_1, back_far = project(dpre, dpre_f, 0, 0)
    for m in (0, 1):
        rs[m][0].scatter_forward(add_into)
    back_2 = relay(0, back_far)
    for m in (2, 3):
        rs[m][1].scatter_forward(add_into)
    for m in (0, 1):
        rs[m][0].scatter_finish(add_into)
        start2(m)
    for m in (2, 3):
        rs[m][1].scatter_finish(add_into)
        z_start(m)
    for m in (0, 1):
        rs[m][1].scatter_forward(add_into)
    for m in (2, 3):
        z_spread(m)
    mixed_1.wait_recv()
    mixed_2.wait_recv()

    def gathered(t, r):
        return mine[t, r, :] + arrived[t, 0, r, :].astype(F32) + arrived[t, 2, r, :].astype(F32)

    @pl.loop(0, patches // chunk)
    def _(i):
        r = pl.ds(pl.multiple_of(i * chunk, chunk), chunk)
        out_ref[r, :] = (resid[r, :].astype(F32) + gathered(1, r)).astype(BF)

    for m in (0, 1):
        rs[m][1].scatter_finish(add_into)
        z_start(m)
    for m in (2, 3):
        z_finish(m)
    for m in (0, 1):
        z_spread(m)
    back_1.wait_recv()
    back_2.wait_recv()

    @pl.loop(0, patches // chunk)
    def _(i):
        r = pl.ds(pl.multiple_of(i * chunk, chunk), chunk)
        _, ahat, rstd = stats(r)
        g = gathered(0, r) * gain
        back = rstd * (
            g
            - jnp.mean(g, axis=-1, keepdims=True)
            - ahat * jnp.mean(g * ahat, axis=-1, keepdims=True)
        )
        grad_ref[r, :] = (cot_ref[r, :].astype(F32) + back).astype(BF)

    for m in (0, 1):
        z_finish(m)
    for m in (2, 3, 0, 1):
        z_last[m].wait_recv()
    sum_ref[...] = total[...]

    for first, second in ag + rs:
        first.drain()
        second.drain()
    for copy in [*z_live.values(), *sends]:
        copy.wait_send()


def layer(q, k, v, tok, cot, gain, io, w, f, nz):
    patches, width = tok.shape
    share = w.shape[1]
    half = share // 2
    hidden = SIDE * SIDE * share
    four = 4 * patches
    nk = nz // 2
    row_groups = min(nk, 2)
    zr, zl = share // row_groups, width // (nk // row_groups)
    vmem = pl.BlockSpec(memory_space=pltpu.VMEM)
    any_space = pl.BlockSpec(memory_space=pl.ANY)
    dma = pltpu.SemaphoreType.DMA
    scratch = [
        pltpu.VMEM((4, SIDE, SIDE, share, width), BF),
        pltpu.VMEM((SIDE, SIDE, *f.shape), F32),
        pltpu.VMEM((4, 8, max(width, 2 * hidden)), F32),
        pltpu.VMEM((4, 8, max(width, 2 * hidden)), F32),
        pltpu.VMEM((four, width), BF),
        pltpu.VMEM((four, width), BF),
        pltpu.VMEM((four, width), BF),
        pltpu.VMEM((four, width), BF),
        pltpu.VMEM((patches, width), BF),
        pltpu.VMEM((four, hidden), BF),
        pltpu.VMEM((four, hidden), BF),
        pltpu.VMEM((four, hidden), F32),
        pltpu.VMEM((four, hidden), BF),
        pltpu.VMEM((four, hidden), BF),
        pltpu.VMEM((2, patches, width), F32),
        pltpu.VMEM((2, 3, patches, width), BF),
        pltpu.VMEM((2, 3, patches, width), BF),
        pltpu.VMEM((4, SIDE, SIDE, share, width), BF),
        pltpu.VMEM((4, 2, SIDE, half, width), BF),
        pltpu.VMEM((4, 4, SIDE, half, width), BF),
        pltpu.VMEM((4, 2, half, width), BF),
        pltpu.VMEM((4, 4, half, width), BF),
        pltpu.VMEM((4, nk - 1, zr, zl), BF),
        pltpu.VMEM((4, 2, 2, share, width), BF),
        dma((60,)),
        dma((60,)),
        dma((48,)),
        dma((48,)),
        dma((4, 2, nz - 1)),
        dma((4, 2, nz - 1)),
        dma((19,)),
        dma((19,)),
        dma((5,)),
    ]
    return pl.pallas_call(
        functools.partial(kernel, nz),
        out_shape=(
            jax.ShapeDtypeStruct((patches, width), BF),
            jax.ShapeDtypeStruct((patches, width), BF),
            jax.ShapeDtypeStruct((4, 2, 2, share, width), BF),
        ),
        in_specs=[vmem] * 7 + [any_space] * 2,
        out_specs=(vmem, vmem, vmem),
        scratch_shapes=scratch,
        compiler_params=pltpu.CompilerParams(
            collective_id=0, has_side_effects=True, vmem_limit_bytes=62 * 1024 * 1024
        ),
        name="layer",
    )(q, k, v, tok, cot, gain, io, w, f)


def body(
    tokens,
    queries,
    keys,
    values,
    ln_gain,
    mean_in,
    sigma_in,
    noise_in,
    mean_out,
    sigma_out,
    noise_out,
    flip_in,
    flip_mid,
    flip_hidden,
    flip_out,
    cotangent,
):
    nz = lax.axis_size("z")
    width = tokens.shape[-1]
    share = mean_in.shape[1] // 4
    quarter = lax.axis_index("c") * 2 + lax.rem(lax.axis_index("z"), 2)
    s = lax.axis_index("x") * SIDE + lax.axis_index("y")
    pert_in = (sigma_in.astype(F32) * noise_in.astype(F32)).astype(BF)
    pert_out = (sigma_out.astype(F32) * noise_out.astype(F32)).astype(BF)

    def own(t, axis):
        return lax.dynamic_slice_in_dim(t, quarter * share, share, axis)

    w = jnp.stack([own(mean_in, 1).T, own(pert_in, 1).T, own(mean_out, 0), own(pert_out, 0)])
    f = jnp.concatenate([flip_mid, flip_hidden], axis=1).astype(F32)
    io = jnp.stack(
        [lax.dynamic_index_in_dim(t, s, 0, False).astype(F32) for t in (flip_in, flip_out)]
    )
    io = jnp.pad(io, ((0, 6), (0, 0)))
    out, grad, sums = layer(
        queries[0], keys[0], values[0], tokens[0], cotangent[0], ln_gain.reshape(1, width), io, w, f, nz
    )
    sums = sums.astype(F32).reshape(4, 4 * share, width)
    grad_mean_in = sums[0].T
    grad_sigma_in = sums[1].T * noise_in.astype(F32)
    grad_mean_out = sums[2]
    grad_sigma_out = sums[3] * noise_out.astype(F32)
    return out[None], grad[None], grad_mean_in, grad_sigma_in, grad_mean_out, grad_sigma_out


def solution(mesh):
    finer = Mesh(mesh.devices.reshape(-1, 2, SIDE, SIDE), ALL)
    images = P(ALL, None, None)
    cols = P(None, SEQ)
    rows = P(SEQ, None)
    in_specs = (
        images,
        images,
        images,
        images,
        P(),
        cols,
        cols,
        cols,
        rows,
        rows,
        rows,
        P(DP, None),
        P(DP, SEQ),
        P(DP, SEQ),
        P(DP, None),
        images,
    )
    out_specs = (images, images, cols, cols, rows, rows)
    return jax.shard_map(body, mesh=finer, in_specs=in_specs, out_specs=out_specs, check_vma=False)
```

```python
import functools

import jax
import jax.numpy as jnp
from jax import lax
from jax.experimental import pallas as pl
from jax.experimental.pallas import tpu as pltpu
from jax.sharding import Mesh
from jax.sharding import PartitionSpec as P

BF = jnp.bfloat16
F32 = jnp.float32
HEAD = 64
SIDE = 4
MESH_ID = pl.DeviceIdType.MESH
DP = ("z", "c")
SEQ = ("x", "y")
ALL = ("z", "c", "x", "y")


def dot_t(a, b):
    return lax.dot_general(a, b, (((1,), (1,)), ((), ())), preferred_element_type=F32)


def dot_0(a, b):
    return lax.dot_general(a, b, (((0,), (0,)), ((), ())), preferred_element_type=F32)


def dot_n(a, b):
    return jnp.dot(a, b, preferred_element_type=F32)


class Ring:
    def __init__(self, at, axis, block, sends, recvs, base):
        me = at[axis]
        self.me = me
        self.right = lax.rem(me + 1, SIDE)
        self.left = lax.rem(me + 3, SIDE)
        self.far = lax.rem(me + 2, SIDE)
        self.block = block
        self.sends, self.recvs, self.base = sends, recvs, base

        def device(pos):
            where = dict(at)
            where[axis] = pos
            return tuple(where[name] for name in ALL)

        self.to_right, self.to_left = device(self.right), device(self.left)
        self.live = {}

    def copy(self, slot, src, dst, right):
        return pltpu.make_async_remote_copy(
            src_ref=src,
            dst_ref=dst,
            send_sem=self.sends.at[self.base + slot],
            recv_sem=self.recvs.at[self.base + slot],
            device_id=self.to_right if right else self.to_left,
            device_id_type=MESH_ID,
        )

    def go(self, slot, src, dst, right):
        copy = self.copy(slot, src, dst, right)
        copy.start()
        self.live[slot] = copy

    def gather_start(self):
        for slot, half, right in ((0, 0, True), (1, 1, False), (2, 1, True), (3, 0, False)):
            ref = self.block(self.me, half)
            self.go(slot, ref, ref, right)

    def gather_forward(self):
        self.live[0].wait_recv()
        ref = self.block(self.left, 0)
        self.go(4, ref, ref, True)
        self.live[1].wait_recv()
        ref = self.block(self.right, 1)
        self.go(5, ref, ref, False)

    def gather_finish(self):
        for slot in (2, 3, 4, 5):
            self.live[slot].wait_recv()

    def scatter_start(self, near, once):
        self.near, self.once = near, once
        self.go(0, self.block(self.far, 0), near[0], True)
        self.go(1, self.block(self.far, 1), near[1], False)
        self.go(2, self.block(self.right, 1), once[1], True)
        self.go(3, self.block(self.left, 0), once[2], False)

    def scatter_forward(self, add):
        self.live[0].wait_recv()
        ref = self.block(self.right, 0)
        add(ref, self.near[0])
        self.go(4, ref, self.once[0], True)
        self.live[1].wait_recv()
        ref = self.block(self.left, 1)
        add(ref, self.near[1])
        self.go(5, ref, self.once[3], False)

    def scatter_finish(self, add):
        for slot in (2, 3, 4, 5):
            self.live[slot].wait_recv()
        add(self.block(self.me, 0), self.once[0], self.once[2])
        add(self.block(self.me, 1), self.once[1], self.once[3])

    def drain(self):
        for slot in sorted(self.live):
            self.live[slot].wait_send()


def add_into(ref, *others):
    if len(ref.shape) == 3:
        for i in range(ref.shape[0]):
            add_into(ref.at[i], *(other.at[i] for other in others))
        return
    total = ref[...].astype(F32)
    for other in others:
        total = total + other[...].astype(F32)
    ref[...] = total.astype(BF)


def kernel(
    nz,
    gain_ref,
    fin_ref,
    fout_ref,
    fmid_ref,
    fhid_ref,
    *refs,
):
    args, refs = refs[:11], refs[11:]
    run(nz, gain_ref, (fin_ref, fout_ref, fmid_ref, fhid_ref), args, *refs)


def run(
    nz,
    gain_ref,
    flips,
    args,
    out_ref,
    grad_ref,
    sum_ref,
    w_all,
    f_all,
    msg,
    signs,
    norm,
    norm_f,
    cot,
    cot_f,
    resid,
    hid,
    hid_f,
    slope,
    dpre,
    dpre_f,
    mine,
    theirs,
    arrived,
    part,
    near1,
    once1,
    near2,
    once2,
    zbuf,
    total,
    ag_s,
    ag_r,
    rs_s,
    rs_r,
    z_s,
    z_r,
    core_s,
    core_r,
    local,
    in_stage,
    out_stage,
    img_stage,
    turned,
    f_ref,
):
    patches, width = out_ref.shape
    share = w_all.shape[3]
    half = share // 2
    own_hidden = SIDE * SIDE * share
    band = min(256, own_hidden)
    per_band = band // (SIDE * share)
    bands = own_hidden // band
    nblk = min(256, width)
    nk = nz // 2
    at = {name: lax.axis_index(name) for name in ALL}
    z, c, x, y = (at[name] for name in ALL)
    s = x * SIDE + y
    zp, zk = lax.rem(z, 2), lax.div(z, 2)
    other = z + 1 - 2 * zp
    partner, mate, cross = (z, 1 - c, x, y), (other, c, x, y), (other, 1 - c, x, y)

    barrier = pltpu.get_barrier_semaphore()
    greet = [
        partner,
        cross,
        *[(lax.rem(z + d, nz), c, x, y) for d in range(1, nz)],
    ]
    plane = [
        (lax.rem(x + d // SIDE, SIDE), lax.rem(y + d % SIDE, SIDE)) for d in range(1, SIDE * SIDE)
    ]
    greet += [(z, c, a, b) for a, b in plane]
    for device in greet:
        pl.semaphore_signal(barrier, inc=1, device_id=device, device_id_type=MESH_ID)

    homes = [*(in_stage.at[i] for i in range(3)), *(out_stage.at[i] for i in range(3))]
    homes += [*(img_stage.at[i] for i in range(4)), cot.at[pl.ds(0, patches)]]
    loads = [pltpu.make_async_copy(arg, home, local.at[i]) for i, (arg, home) in enumerate(zip(args, homes))]
    for load in loads:
        load.start()
    q_ref, k_ref, v_ref, tok_ref = (img_stage.at[i] for i in range(4))
    cot_ref = cot.at[pl.ds(0, patches)]
    fin_ref, fout_ref, fmid_ref, fhid_ref = flips
    images = fin_ref.shape[0]
    for kind, ref in enumerate((fmid_ref, fhid_ref)):
        table = ref[...].astype(F32)
        for i in range(images):
            f_ref[i, kind : kind + 1, :] = table[i : i + 1, :]
    for load in loads[:6]:
        load.wait()
    mine_rows = pl.ds(pl.multiple_of((2 * c + zp) * share, share), share)
    turned[0] = in_stage[0].T
    turned[1] = (in_stage[1].astype(F32) * in_stage[2].astype(F32)).astype(BF).T
    turned[2] = (out_stage[1].astype(F32) * out_stage[2].astype(F32)).astype(BF)
    w_all[0, x, y] = turned[0, mine_rows, :]
    w_all[1, x, y] = turned[1, mine_rows, :]
    w_all[2, x, y] = out_stage[0, mine_rows, :]
    w_all[3, x, y] = turned[2, mine_rows, :]
    f_all[x, y] = f_ref[s]
    for load in loads[6:]:
        load.wait()

    def attend(p):
        lanes = pl.ds(pl.multiple_of(p * 128, 128), 128)
        q2, k2, v2 = q_ref[:, lanes], k_ref[:, lanes], v_ref[:, lanes]
        outs = []
        for i in range(2):
            cols = slice(i * HEAD, (i + 1) * HEAD)
            scores = dot_t(q2[:, cols], k2[:, cols]) * (HEAD**-0.5)
            e = jnp.exp(scores - jnp.max(scores, axis=-1, keepdims=True))
            norm_by = jnp.sum(e, axis=-1, keepdims=True)
            outs.append(dot_n(e.astype(BF), v2[:, cols]) / norm_by)
        attn = jnp.concatenate(outs, axis=1).astype(BF)
        resid[:, lanes] = (tok_ref[:, lanes].astype(F32) + attn.astype(F32)).astype(BF)

    pairs = width // 128

    def attend_span(k):
        @pl.loop(k * pairs // 4, (k + 1) * pairs // 4)
        def _(p):
            attend(p)

    attend_span(0)
    pl.semaphore_wait(barrier, len(greet))

    def remote(slot, src, dst, device):
        return pltpu.make_async_remote_copy(
            src_ref=src,
            dst_ref=dst,
            send_sem=core_s.at[slot],
            recv_sem=core_r.at[slot],
            device_id=device,
            device_id_type=MESH_ID,
        )

    def halves(n):
        return lambda h: pl.ds(h * n, n)

    rows_of = halves(half)

    def gather_rings(m, base):
        if m % 2 == 0:
            first = Ring(at, "x", lambda j, h: w_all.at[m, j, y, rows_of(h)], ag_s, ag_r, base)
            second = Ring(at, "y", lambda j, h: w_all.at[m, :, j, rows_of(h)], ag_s, ag_r, base + 6)
        else:
            first = Ring(at, "y", lambda j, h: w_all.at[m, x, j, rows_of(h)], ag_s, ag_r, base)
            second = Ring(at, "x", lambda j, h: w_all.at[m, j, :, rows_of(h)], ag_s, ag_r, base + 6)
        return first, second

    def slot_rows(i):
        return pl.ds(i * patches, patches)

    ag = [gather_rings(m, 12 * m) for m in range(4)]
    sends = []

    def send(src, dst, device):
        copy = remote(len(sends), src, dst, device)
        copy.start()
        sends.append(copy)
        return copy

    for m in (0, 1):
        ag[m][0].gather_start()
    half_rows = [pl.ds(h * (patches // 2), patches // 2) for h in range(2)]

    def half_slot(i, h):
        return cot.at[pl.ds(i * patches + h * (patches // 2), patches // 2)]

    cot_2 = [send(cot_ref.at[half_rows[0]], half_slot(2, 0), mate)]
    tables = [
        send(f_ref.at[a * SIDE + b], f_all.at[x, y], (z, c, a, b)) for a, b in plane
    ]
    for m in (2, 3):
        ag[m][0].gather_start()
    cot_1 = send(cot_ref, cot.at[slot_rows(1)], partner)

    attend_span(1)
    for m in (0, 1):
        ag[m][0].gather_forward()
    attend_span(2)
    for m in (2, 3):
        ag[m][0].gather_forward()
    for m in (0, 1):
        ag[m][0].gather_finish()
        ag[m][1].gather_start()

    for copy in tables:
        copy.wait_recv()
    def own_row(t):
        keep = lax.broadcasted_iota(jnp.int32, t.shape, 0) == s
        return jnp.sum(jnp.where(keep, t.astype(F32), 0.0), axis=0, keepdims=True)

    for row, ref in enumerate((fin_ref, fout_ref)):
        own = own_row(ref[...])
        for t in range(4):
            msg[t, row : row + 1, 0:width] = own
    for a in range(SIDE):
        picked = [f_all[a, b] for b in range(SIDE)]
        for t in range(4):
            for kind in range(2):
                lo = t * share
                first = kind * own_hidden + a * SIDE * share
                msg[t, 2:3, first : first + SIDE * share] = jnp.concatenate(
                    [row[kind : kind + 1, lo : lo + share] for row in picked], axis=1
                )
    quarter = lambda core, parity: msg.at[2 * core + parity]
    sign_1 = send(quarter(1 - c, zp), signs.at[1], partner)
    sign_2 = send(quarter(c, 1 - zp), signs.at[2], mate)
    sign_3 = send(quarter(1 - c, 1 - zp), signs.at[3], cross)
    signs[0] = msg[2 * c + zp]

    attend_span(3)

    chunk = min(64, patches)
    gain = gain_ref[...].astype(F32).reshape(1, width)

    def stats(r):
        xf = resid[r, :].astype(F32)
        centered = xf - jnp.mean(xf, axis=-1, keepdims=True)
        rstd = lax.rsqrt(jnp.mean(centered * centered, axis=-1, keepdims=True) + 1e-06)
        return xf, centered * rstd, rstd

    @pl.loop(0, patches // chunk)
    def _(i):
        r = pl.ds(pl.multiple_of(i * chunk, chunk), chunk)
        _, ahat, _ = stats(r)
        norm[r, :] = (ahat * gain).astype(BF)

    norm_1 = send(norm.at[slot_rows(0)], norm.at[slot_rows(1)], partner)
    norm_2 = send(norm.at[slot_rows(0)], norm.at[slot_rows(2)], mate)
    cot_2.append(send(cot_ref.at[half_rows[1]], half_slot(2, 1), mate))
    for m in (2, 3):
        ag[m][0].gather_finish()

    def flip(dst, src, slot, row):
        @pl.loop(0, patches // chunk)
        def _(i):
            r = pl.ds(pl.multiple_of(slot * patches + i * chunk, chunk), chunk)
            dst[r, :] = src[r, :] * signs[slot, row : row + 1, 0:width].astype(BF)

    flip(norm_f, norm, 0, 0)
    flip(cot_f, cot, 0, 1)
    for m in (0, 1):
        ag[m][1].gather_forward()
    for m in (2, 3):
        ag[m][1].gather_start()
    for copy in (cot_1, norm_1, sign_1):
        copy.wait_recv()
    flip(norm_f, norm, 1, 0)
    flip(cot_f, cot, 1, 1)
    cot_2[0].wait_recv()
    cot_3 = [send(half_slot(2, 0), half_slot(3, 0), partner)]
    for m in (0, 1):
        ag[m][1].gather_finish()

    def weight(m, h):
        return w_all[m, pl.ds(h * per_band, per_band)].reshape(band, width)

    def spans(t):
        i, h = lax.div(t, bands), lax.rem(t, bands)
        return (
            i,
            h,
            pl.ds(pl.multiple_of(i * patches, patches), patches),
            pl.ds(pl.multiple_of(h * band, band), band),
        )

    def hidden_row(i, h):
        return signs[i, 2:3, pl.ds(pl.multiple_of(own_hidden + h * band, band), band)]

    def forward(first, last):
        @pl.loop(first * bands, last * bands)
        def _(t):
            i, h, r, lanes = spans(t)
            pre = dot_t(norm[r, :], weight(0, h))
            pre = pre + dot_t(norm_f[r, :], weight(1, h)) * signs[i, 2:3, lanes]
            cdf = 0.5 * (1.0 + lax.erf(pre * 0.7071067811865476))
            pdf = jnp.exp(-0.5 * pre * pre) * 0.3989422804014327
            slope[r, lanes] = cdf + pre * pdf
            unit = (pre * cdf).astype(BF)
            hid[r, lanes] = unit
            hid_f[r, lanes] = unit * hidden_row(i, h).astype(BF)

    def backward(first, last):
        @pl.loop(first * bands, last * bands)
        def _(t):
            i, h, r, lanes = spans(t)
            dh = dot_t(cot[r, :], weight(2, h))
            dh = dh + dot_t(cot_f[r, :], weight(3, h)) * hidden_row(i, h)
            unit = (dh * slope[r, lanes]).astype(BF)
            dpre[r, lanes] = unit
            dpre_f[r, lanes] = unit * signs[i, 2:3, lanes].astype(BF)

    def weight_grad(m, left, right):
        @pl.loop(0, bands)
        def _(h):
            lhs = left[:, pl.ds(pl.multiple_of(h * band, band), band)]
            for n in range(width // nblk):
                cols = slice(n * nblk, (n + 1) * nblk)
                part[m, pl.ds(h * per_band, per_band), :, :, cols] = (
                    dot_0(lhs, right[:, cols]).astype(BF).reshape(per_band, SIDE, share, nblk)
                )

    def scatter_rings(m, base):
        along_y = lambda j, h: part.at[m, :, j, rows_of(h)]
        along_x = lambda j, h: part.at[m, j, :, rows_of(h)]
        one = lambda j, h: part.at[m, j, y, rows_of(h)]
        two = lambda j, h: part.at[m, x, j, rows_of(h)]
        if m % 2 == 0:
            return Ring(at, "y", along_y, rs_s, rs_r, base), Ring(at, "x", one, rs_s, rs_r, base + 6)
        return Ring(at, "x", along_x, rs_s, rs_r, base), Ring(at, "y", two, rs_s, rs_r, base + 6)

    rs = [scatter_rings(m, 12 * m) for m in range(4)]

    def start1(m):
        rs[m][0].scatter_start([near1.at[m, k] for k in range(2)], [once1.at[m, k] for k in range(4)])

    def start2(m):
        rs[m][1].scatter_start([near2.at[m, k] for k in range(2)], [once2.at[m, k] for k in range(4)])

    row_groups = min(nk, 2)
    lane_groups = nk // row_groups
    zr, zl = share // row_groups, width // lane_groups

    def spot(j):
        return (
            pl.ds(pl.multiple_of(lax.div(j, lane_groups) * zr, zr), zr),
            pl.ds(pl.multiple_of(lax.rem(j, lane_groups) * zl, zl), zl),
        )

    z_live = {}

    def z_copy(m, stage, d, step, src, dst):
        copy = pltpu.make_async_remote_copy(
            src_ref=src,
            dst_ref=dst,
            send_sem=z_s.at[m, stage, d - 1],
            recv_sem=z_r.at[m, stage, d - 1],
            device_id=(lax.rem(z + step * d, nz), c, x, y),
            device_id_type=MESH_ID,
        )
        copy.start()
        z_live[m, stage, d] = copy

    def z_start(m):
        for d in range(1, nk):
            r, l = spot(lax.rem(zk + d, nk))
            z_copy(m, 0, d, 2, part.at[m, x, y, r, l], zbuf.at[m, d - 1])

    def z_spread(m):
        r, l = spot(zk)
        acc = part[m, x, y, r, l].astype(F32)
        for d in range(1, nk):
            z_live[m, 0, d].wait_recv()
            acc = acc + zbuf[m, d - 1].astype(F32)
        total[m, c, zp, r, l] = acc.astype(BF)
        for d in range(1, nk):
            place = total.at[m, c, zp, r, l]
            z_copy(m, 1, d, 2, place, place)

    beside = (lax.rem(z + nz - 1 + 2 * zp, nz), c, x, y)
    last = {}

    def z_hand(m):
        for d in range(1, nk):
            z_live[m, 1, d].wait_recv()
        own = total.at[m, c, zp]
        last[m, 0] = send(own, own, beside)
        last[m, 1] = send(own, own, partner)

    def z_finish(m):
        last[m, 0].wait_recv()
        far = total.at[m, c, 1 - zp]
        last[m, 2] = send(far, far, partner)

    def project(left, left_f, t, sign, slots):
        m = 2 * t

        @pl.loop(0, width // nblk)
        def _(n):
            lanes = pl.ds(pl.multiple_of(n * nblk, nblk), nblk)
            plain = w_all[m, :, :, :, lanes].reshape(own_hidden, nblk)
            noisy = w_all[m + 1, :, :, :, lanes].reshape(own_hidden, nblk)
            for i in slots:
                r = slice(i * patches, (i + 1) * patches)
                out = dot_n(left[r, :], plain)
                out = out + dot_n(left_f[r, :], noisy) * signs[i, sign : sign + 1, lanes]
                if i:
                    theirs[t, i - 1, :, lanes] = out.astype(BF)
                else:
                    mine[t, :, lanes] = out

    def relay(t, to_far):
        to_far.wait_recv()

        @pl.loop(0, patches // chunk)
        def _(i):
            r = pl.ds(pl.multiple_of(i * chunk, chunk), chunk)
            both = theirs[t, 1, r, :].astype(F32) + arrived[t, 1, r, :].astype(F32)
            theirs[t, 1, r, :] = both.astype(BF)

        return send(theirs.at[t, 1], arrived.at[t, 2], mate)

    forward(0, 2)
    for m in (2, 3):
        ag[m][1].gather_forward()
    sign_2.wait_recv()
    norm_2.wait_recv()
    norm_3 = send(norm.at[slot_rows(2)], norm.at[slot_rows(3)], partner)
    flip(norm_f, norm, 2, 0)
    forward(2, 3)
    sign_3.wait_recv()
    norm_3.wait_recv()
    flip(norm_f, norm, 3, 0)
    forward(3, 4)
    for m in (2, 3):
        ag[m][1].gather_finish()
    project(hid, hid_f, 1, 1, (2, 3))
    mixed_far = send(theirs.at[1, 2], arrived.at[1, 1], partner)
    cot_2[1].wait_recv()
    cot_3.append(send(half_slot(2, 1), half_slot(3, 1), partner))
    flip(cot_f, cot, 2, 1)
    mixed_2 = relay(1, mixed_far)
    for copy in cot_3:
        copy.wait_recv()
    flip(cot_f, cot, 3, 1)
    weight_grad(2, hid, cot)
    start1(2)
    weight_grad(3, hid_f, cot_f)
    start1(3)
    backward(0, 4)
    rs[2][0].scatter_forward(add_into)
    weight_grad(0, dpre, norm)
    start1(0)
    rs[3][0].scatter_forward(add_into)
    weight_grad(1, dpre_f, norm_f)
    start1(1)
    project(dpre, dpre_f, 0, 0, (2, 3))
    back_far = send(theirs.at[0, 2], arrived.at[0, 1], partner)

    def finish1(m):
        rs[m][0].scatter_finish(add_into)
        start2(m)

    def forward1(m):
        rs[m][0].scatter_forward(add_into)

    def forward2(m):
        rs[m][1].scatter_forward(add_into)

    def finish2(m):
        rs[m][1].scatter_finish(add_into)
        z_start(m)

    def gathered(t, r):
        return mine[t, r, :] + arrived[t, 0, r, :].astype(F32) + arrived[t, 2, r, :].astype(F32)

    finish1(2)
    back_2 = relay(0, back_far)
    finish1(3)
    project(hid, hid_f, 1, 1, (0, 1))
    mixed_1 = send(theirs.at[1, 0], arrived.at[1, 0], partner)
    forward1(0)
    forward2(2)
    project(dpre, dpre_f, 0, 0, (0, 1))
    back_1 = send(theirs.at[0, 0], arrived.at[0, 0], partner)
    forward2(3)
    forward1(1)
    finish2(2)
    finish2(3)
    finish1(0)
    mixed_1.wait_recv()
    mixed_2.wait_recv()

    @pl.loop(0, patches // chunk)
    def _(i):
        r = pl.ds(pl.multiple_of(i * chunk, chunk), chunk)
        out_ref[r, :] = (resid[r, :].astype(F32) + gathered(1, r)).astype(BF)

    finish1(1)
    forward2(0)
    forward2(1)
    finish2(0)
    finish2(1)
    z_spread(2)
    z_spread(3)
    z_spread(0)
    z_spread(1)
    back_1.wait_recv()
    back_2.wait_recv()

    @pl.loop(0, patches // chunk)
    def _(i):
        r = pl.ds(pl.multiple_of(i * chunk, chunk), chunk)
        _, ahat, rstd = stats(r)
        g = gathered(0, r) * gain
        back = rstd * (
            g
            - jnp.mean(g, axis=-1, keepdims=True)
            - ahat * jnp.mean(g * ahat, axis=-1, keepdims=True)
        )
        grad_ref[r, :] = (cot_ref[r, :].astype(F32) + back).astype(BF)

    for m in (2, 3, 0, 1):
        z_hand(m)
    z_finish(2)
    z_finish(3)
    for m in (2, 3):
        last[m, 1].wait_recv()
        last[m, 2].wait_recv()
        sum_ref[m] = total[m]
    z_finish(0)
    z_finish(1)
    for m in (0, 1):
        last[m, 1].wait_recv()
        last[m, 2].wait_recv()
        sum_ref[m] = total[m]

    for first, second in ag + rs:
        first.drain()
        second.drain()
    for copy in [*z_live.values(), *sends]:
        copy.wait_send()


def layer(gain, flips, mats, images, nz):
    patches, width = images[0].shape
    cols = mats[0].shape[1]
    share = cols // 4
    count = flips[0].shape[0]
    half = share // 2
    hidden = SIDE * SIDE * share
    four = 4 * patches
    nk = nz // 2
    row_groups = min(nk, 2)
    zr, zl = share // row_groups, width // (nk // row_groups)
    vmem = pl.BlockSpec(memory_space=pltpu.VMEM)
    any_space = pl.BlockSpec(memory_space=pl.ANY)
    dma = pltpu.SemaphoreType.DMA
    scratch = [
        pltpu.VMEM((4, SIDE, SIDE, share, width), BF),
        pltpu.VMEM((SIDE, SIDE, 8, cols), F32),
        pltpu.VMEM((4, 8, max(width, 2 * hidden)), F32),
        pltpu.VMEM((4, 8, max(width, 2 * hidden)), F32),
        pltpu.VMEM((four, width), BF),
        pltpu.VMEM((four, width), BF),
        pltpu.VMEM((four, width), BF),
        pltpu.VMEM((four, width), BF),
        pltpu.VMEM((patches, width), BF),
        pltpu.VMEM((four, hidden), BF),
        pltpu.VMEM((four, hidden), BF),
        pltpu.VMEM((four, hidden), F32),
        pltpu.VMEM((four, hidden), BF),
        pltpu.VMEM((four, hidden), BF),
        pltpu.VMEM((2, patches, width), F32),
        pltpu.VMEM((2, 3, patches, width), BF),
        pltpu.VMEM((2, 3, patches, width), BF),
        pltpu.VMEM((4, SIDE, SIDE, share, width), BF),
        pltpu.VMEM((4, 2, SIDE, half, width), BF),
        pltpu.VMEM((4, 4, SIDE, half, width), BF),
        pltpu.VMEM((4, 2, half, width), BF),
        pltpu.VMEM((4, 4, half, width), BF),
        pltpu.VMEM((4, nk - 1, zr, zl), BF),
        pltpu.VMEM((4, 2, 2, share, width), BF),
        dma((48,)),
        dma((48,)),
        dma((48,)),
        dma((48,)),
        dma((4, 2, nk - 1)),
        dma((4, 2, nk - 1)),
        dma((44,)),
        dma((44,)),
        dma((11,)),
        pltpu.VMEM((3, width, cols), BF),
        pltpu.VMEM((3, cols, width), BF),
        pltpu.VMEM((4, patches, width), BF),
        pltpu.VMEM((3, cols, width), BF),
        pltpu.VMEM((count, 8, cols), F32),
    ]
    return pl.pallas_call(
        functools.partial(kernel, nz),
        out_shape=(
            jax.ShapeDtypeStruct((patches, width), BF),
            jax.ShapeDtypeStruct((patches, width), BF),
            jax.ShapeDtypeStruct((4, 2, 2, share, width), BF),
        ),
        in_specs=[vmem] * 5 + [any_space] * 11,
        out_specs=(vmem, vmem, vmem),
        scratch_shapes=scratch,
        compiler_params=pltpu.CompilerParams(
            collective_id=0, has_side_effects=True, vmem_limit_bytes=62 * 1024 * 1024
        ),
        name="layer",
    )(gain, *flips, *mats, *images)


def body(
    tokens,
    queries,
    keys,
    values,
    ln_gain,
    mean_in,
    sigma_in,
    noise_in,
    mean_out,
    sigma_out,
    noise_out,
    flip_in,
    flip_mid,
    flip_hidden,
    flip_out,
    cotangent,
):
    nz = lax.axis_size("z")
    width = tokens.shape[-1]
    cols = mean_in.shape[1]
    out, grad, sums = layer(
        ln_gain,
        (flip_in, flip_out, flip_mid, flip_hidden),
        (mean_in, sigma_in, noise_in, mean_out, sigma_out, noise_out),
        (queries[0], keys[0], values[0], tokens[0], cotangent[0]),
        nz,
    )
    sums = sums.astype(F32).reshape(4, cols, width)
    grad_mean_in = sums[0].T
    grad_sigma_in = sums[1].T * noise_in.astype(F32)
    grad_mean_out = sums[2]
    grad_sigma_out = sums[3] * noise_out.astype(F32)
    return out[None], grad[None], grad_mean_in, grad_sigma_in, grad_mean_out, grad_sigma_out


def solution(mesh):
    finer = Mesh(mesh.devices.reshape(-1, 2, SIDE, SIDE), ALL)
    images = P(ALL, None, None)
    cols = P(None, SEQ)
    rows = P(SEQ, None)
    in_specs = (
        images,
        images,
        images,
        images,
        P(),
        cols,
        cols,
        cols,
        rows,
        rows,
        rows,
        P(DP, None),
        P(DP, SEQ),
        P(DP, SEQ),
        P(DP, None),
        images,
    )
    out_specs = (images, images, cols, cols, rows, rows)
    return jax.shard_map(body, mesh=finer, in_specs=in_specs, out_specs=out_specs, check_vma=False)
```

```python
import functools

import jax
import jax.numpy as jnp
from jax import lax
from jax.experimental import pallas as pl
from jax.experimental.pallas import tpu as pltpu
from jax.sharding import Mesh
from jax.sharding import PartitionSpec as P

BF = jnp.bfloat16
F32 = jnp.float32
HEAD = 64
SIDE = 4
MESH_ID = pl.DeviceIdType.MESH
DP = ("z", "c")
SEQ = ("x", "y")
ALL = ("z", "c", "x", "y")


def dot_t(a, b):
    return lax.dot_general(a, b, (((1,), (1,)), ((), ())), preferred_element_type=F32)


def dot_0(a, b):
    return lax.dot_general(a, b, (((0,), (0,)), ((), ())), preferred_element_type=F32)


def dot_n(a, b):
    return jnp.dot(a, b, preferred_element_type=F32)


class Ring:
    def __init__(self, at, axis, block, sends, recvs, base):
        me = at[axis]
        self.me = me
        self.right = lax.rem(me + 1, SIDE)
        self.left = lax.rem(me + 3, SIDE)
        self.far = lax.rem(me + 2, SIDE)
        self.block = block
        self.sends, self.recvs, self.base = sends, recvs, base

        def device(pos):
            where = dict(at)
            where[axis] = pos
            return tuple(where[name] for name in ALL)

        self.to_right, self.to_left = device(self.right), device(self.left)
        self.live = {}

    def copy(self, slot, src, dst, right):
        return pltpu.make_async_remote_copy(
            src_ref=src,
            dst_ref=dst,
            send_sem=self.sends.at[self.base + slot],
            recv_sem=self.recvs.at[self.base + slot],
            device_id=self.to_right if right else self.to_left,
            device_id_type=MESH_ID,
        )

    def go(self, slot, src, dst, right):
        copy = self.copy(slot, src, dst, right)
        copy.start()
        self.live[slot] = copy

    def gather_start(self):
        for slot, half, right in ((0, 0, True), (1, 1, False), (2, 1, True), (3, 0, False)):
            ref = self.block(self.me, half)
            self.go(slot, ref, ref, right)

    def gather_forward(self):
        self.live[0].wait_recv()
        ref = self.block(self.left, 0)
        self.go(4, ref, ref, True)
        self.live[1].wait_recv()
        ref = self.block(self.right, 1)
        self.go(5, ref, ref, False)

    def gather_finish(self):
        for slot in (2, 3, 4, 5):
            self.live[slot].wait_recv()

    def scatter_start(self, near, once):
        self.near, self.once = near, once
        self.go(0, self.block(self.far, 0), near[0], True)
        self.go(1, self.block(self.far, 1), near[1], False)
        self.go(2, self.block(self.right, 1), once[1], True)
        self.go(3, self.block(self.left, 0), once[2], False)

    def scatter_forward(self, add):
        self.live[0].wait_recv()
        ref = self.block(self.right, 0)
        add(ref, self.near[0])
        self.go(4, ref, self.once[0], True)
        self.live[1].wait_recv()
        ref = self.block(self.left, 1)
        add(ref, self.near[1])
        self.go(5, ref, self.once[3], False)

    def scatter_finish(self, add):
        for slot in (2, 3, 4, 5):
            self.live[slot].wait_recv()
        add(self.block(self.me, 0), self.once[0], self.once[2])
        add(self.block(self.me, 1), self.once[1], self.once[3])

    def drain(self):
        for slot in sorted(self.live):
            self.live[slot].wait_send()


def add_into(ref, *others):
    if len(ref.shape) == 3:
        for i in range(ref.shape[0]):
            add_into(ref.at[i], *(other.at[i] for other in others))
        return
    total = ref[...].astype(F32)
    for other in others:
        total = total + other[...].astype(F32)
    ref[...] = total.astype(BF)


def kernel(
    nz,
    gain_ref,
    fin_ref,
    fout_ref,
    fmid_ref,
    fhid_ref,
    *refs,
):
    args, refs = refs[:11], refs[11:]
    run(nz, gain_ref, (fin_ref, fout_ref, fmid_ref, fhid_ref), args, *refs)


def run(
    nz,
    gain_ref,
    flips,
    args,
    out_ref,
    grad_ref,
    mean_in_ref,
    sigma_in_ref,
    mean_out_ref,
    sigma_out_ref,
    w_all,
    f_all,
    msg,
    signs,
    norm,
    norm_f,
    cot,
    cot_f,
    resid,
    hid,
    hid_f,
    slope,
    dpre,
    dpre_f,
    mine,
    theirs,
    arrived,
    part,
    near1,
    once1,
    near2,
    once2,
    zbuf,
    total,
    ag_s,
    ag_r,
    rs_s,
    rs_r,
    z_s,
    z_r,
    core_s,
    core_r,
    local,
    in_stage,
    out_stage,
    img_stage,
    turned,
    f_ref,
):
    patches, width = out_ref.shape
    share = w_all.shape[3]
    half = share // 2
    own_hidden = SIDE * SIDE * share
    band = min(256, own_hidden)
    per_band = band // (SIDE * share)
    bands = own_hidden // band
    nblk = min(256, width)
    nk = nz // 2
    at = {name: lax.axis_index(name) for name in ALL}
    z, c, x, y = (at[name] for name in ALL)
    s = x * SIDE + y
    zp, zk = lax.rem(z, 2), lax.div(z, 2)
    other = z + 1 - 2 * zp
    partner, mate, cross = (z, 1 - c, x, y), (other, c, x, y), (other, 1 - c, x, y)

    barrier = pltpu.get_barrier_semaphore()
    greet = [
        partner,
        cross,
        *[(lax.rem(z + d, nz), c, x, y) for d in range(1, nz)],
    ]
    plane = [
        (lax.rem(x + d // SIDE, SIDE), lax.rem(y + d % SIDE, SIDE)) for d in range(1, SIDE * SIDE)
    ]
    greet += [(z, c, a, b) for a, b in plane]
    for device in greet:
        pl.semaphore_signal(barrier, inc=1, device_id=device, device_id_type=MESH_ID)

    homes = [*(in_stage.at[i] for i in range(3)), *(out_stage.at[i] for i in range(3))]
    homes += [*(img_stage.at[i] for i in range(4)), cot.at[pl.ds(0, patches)]]
    loads = [pltpu.make_async_copy(arg, home, local.at[i]) for i, (arg, home) in enumerate(zip(args, homes))]
    for load in loads:
        load.start()
    q_ref, k_ref, v_ref, tok_ref = (img_stage.at[i] for i in range(4))
    cot_ref = cot.at[pl.ds(0, patches)]
    fin_ref, fout_ref, fmid_ref, fhid_ref = flips
    images = fin_ref.shape[0]
    for kind, ref in enumerate((fmid_ref, fhid_ref)):
        table = ref[...].astype(F32)
        for i in range(images):
            f_ref[i, kind : kind + 1, :] = table[i : i + 1, :]
    for load in loads[:6]:
        load.wait()
    mine_rows = pl.ds(pl.multiple_of((2 * c + zp) * share, share), share)
    turned[0] = in_stage[0].T
    turned[1] = (in_stage[1].astype(F32) * in_stage[2].astype(F32)).astype(BF).T
    turned[2] = (out_stage[1].astype(F32) * out_stage[2].astype(F32)).astype(BF)
    w_all[0, x, y] = turned[0, mine_rows, :]
    w_all[1, x, y] = turned[1, mine_rows, :]
    w_all[2, x, y] = out_stage[0, mine_rows, :]
    w_all[3, x, y] = turned[2, mine_rows, :]
    f_all[x, y] = f_ref[s]
    for load in loads[6:]:
        load.wait()

    def attend(p):
        lanes = pl.ds(pl.multiple_of(p * 128, 128), 128)
        q2, k2, v2 = q_ref[:, lanes], k_ref[:, lanes], v_ref[:, lanes]
        outs = []
        for i in range(2):
            cols = slice(i * HEAD, (i + 1) * HEAD)
            scores = dot_t(q2[:, cols], k2[:, cols]) * (HEAD**-0.5)
            e = jnp.exp(scores - jnp.max(scores, axis=-1, keepdims=True))
            norm_by = jnp.sum(e, axis=-1, keepdims=True)
            outs.append(dot_n(e.astype(BF), v2[:, cols]) / norm_by)
        attn = jnp.concatenate(outs, axis=1).astype(BF)
        resid[:, lanes] = (tok_ref[:, lanes].astype(F32) + attn.astype(F32)).astype(BF)

    pairs = width // 128

    def attend_span(k):
        @pl.loop(k * pairs // 4, (k + 1) * pairs // 4)
        def _(p):
            attend(p)

    attend_span(0)
    pl.semaphore_wait(barrier, len(greet))

    def remote(slot, src, dst, device):
        return pltpu.make_async_remote_copy(
            src_ref=src,
            dst_ref=dst,
            send_sem=core_s.at[slot],
            recv_sem=core_r.at[slot],
            device_id=device,
            device_id_type=MESH_ID,
        )

    def halves(n):
        return lambda h: pl.ds(h * n, n)

    rows_of = halves(half)

    def gather_rings(m, base):
        if m % 2 == 0:
            first = Ring(at, "x", lambda j, h: w_all.at[m, j, y, rows_of(h)], ag_s, ag_r, base)
            second = Ring(at, "y", lambda j, h: w_all.at[m, :, j, rows_of(h)], ag_s, ag_r, base + 6)
        else:
            first = Ring(at, "y", lambda j, h: w_all.at[m, x, j, rows_of(h)], ag_s, ag_r, base)
            second = Ring(at, "x", lambda j, h: w_all.at[m, j, :, rows_of(h)], ag_s, ag_r, base + 6)
        return first, second

    def slot_rows(i):
        return pl.ds(i * patches, patches)

    ag = [gather_rings(m, 12 * m) for m in range(4)]
    sends = []

    def send(src, dst, device):
        copy = remote(len(sends), src, dst, device)
        copy.start()
        sends.append(copy)
        return copy

    tables = [
        send(f_ref.at[a * SIDE + b], f_all.at[x, y], (z, c, a, b)) for a, b in plane
    ]
    for m in range(4):
        ag[m][0].gather_start()
    half_rows = [pl.ds(h * (patches // 2), patches // 2) for h in range(2)]

    def half_slot(i, h):
        return cot.at[pl.ds(i * patches + h * (patches // 2), patches // 2)]

    cot_2 = [send(cot_ref.at[half_rows[0]], half_slot(2, 0), mate)]
    cot_1 = send(cot_ref, cot.at[slot_rows(1)], partner)

    attend_span(1)
    attend_span(2)
    for m in (0, 1):
        ag[m][0].gather_forward()
    attend_span(3)
    for m in (2, 3):
        ag[m][0].gather_forward()

    chunk = min(64, patches)
    gain = gain_ref[...].astype(F32).reshape(1, width)

    def stats(r):
        xf = resid[r, :].astype(F32)
        centered = xf - jnp.mean(xf, axis=-1, keepdims=True)
        rstd = lax.rsqrt(jnp.mean(centered * centered, axis=-1, keepdims=True) + 1e-06)
        return xf, centered * rstd, rstd

    @pl.loop(0, patches // chunk)
    def _(i):
        r = pl.ds(pl.multiple_of(i * chunk, chunk), chunk)
        _, ahat, _ = stats(r)
        norm[r, :] = (ahat * gain).astype(BF)

    norm_1 = send(norm.at[slot_rows(0)], norm.at[slot_rows(1)], partner)
    norm_2 = send(norm.at[slot_rows(0)], norm.at[slot_rows(2)], mate)
    for m in (0, 1):
        ag[m][0].gather_finish()
        ag[m][1].gather_start()

    for copy in tables:
        copy.wait_recv()
    def own_row(t):
        keep = lax.broadcasted_iota(jnp.int32, t.shape, 0) == s
        return jnp.sum(jnp.where(keep, t.astype(F32), 0.0), axis=0, keepdims=True)

    for row, ref in enumerate((fin_ref, fout_ref)):
        own = own_row(ref[...])
        for t in range(4):
            msg[t, row : row + 1, 0:width] = own
    for a in range(SIDE):
        picked = [f_all[a, b] for b in range(SIDE)]
        for t in range(4):
            for kind in range(2):
                lo = t * share
                first = kind * own_hidden + a * SIDE * share
                msg[t, 2:3, first : first + SIDE * share] = jnp.concatenate(
                    [row[kind : kind + 1, lo : lo + share] for row in picked], axis=1
                )
    quarter = lambda core, parity: msg.at[2 * core + parity]
    sign_1 = send(quarter(1 - c, zp), signs.at[1], partner)
    sign_2 = send(quarter(c, 1 - zp), signs.at[2], mate)
    sign_3 = send(quarter(1 - c, 1 - zp), signs.at[3], cross)
    signs[0] = msg[2 * c + zp]
    cot_2.append(send(cot_ref.at[half_rows[1]], half_slot(2, 1), mate))

    def flip(dst, src, slot, row):
        @pl.loop(0, patches // chunk)
        def _(i):
            r = pl.ds(pl.multiple_of(slot * patches + i * chunk, chunk), chunk)
            dst[r, :] = src[r, :] * signs[slot, row : row + 1, 0:width].astype(BF)

    flip(norm_f, norm, 0, 0)
    flip(cot_f, cot, 0, 1)
    for m in (2, 3):
        ag[m][0].gather_finish()
    for m in (0, 1):
        ag[m][1].gather_forward()
    for m in (2, 3):
        ag[m][1].gather_start()
    for copy in (cot_1, norm_1, sign_1):
        copy.wait_recv()
    flip(norm_f, norm, 1, 0)
    flip(cot_f, cot, 1, 1)
    cot_2[0].wait_recv()
    cot_3 = [send(half_slot(2, 0), half_slot(3, 0), partner)]
    for m in (0, 1):
        ag[m][1].gather_finish()

    def weight(m, h):
        return w_all[m, pl.ds(h * per_band, per_band)].reshape(band, width)

    def spans(t):
        i, h = lax.div(t, bands), lax.rem(t, bands)
        return (
            i,
            h,
            pl.ds(pl.multiple_of(i * patches, patches), patches),
            pl.ds(pl.multiple_of(h * band, band), band),
        )

    def hidden_row(i, h):
        return signs[i, 2:3, pl.ds(pl.multiple_of(own_hidden + h * band, band), band)]

    def forward(first, last):
        @pl.loop(first * bands, last * bands)
        def _(t):
            i, h, r, lanes = spans(t)
            pre = dot_t(norm[r, :], weight(0, h))
            pre = pre + dot_t(norm_f[r, :], weight(1, h)) * signs[i, 2:3, lanes]
            cdf = 0.5 * (1.0 + lax.erf(pre * 0.7071067811865476))
            pdf = jnp.exp(-0.5 * pre * pre) * 0.3989422804014327
            slope[r, lanes] = cdf + pre * pdf
            unit = (pre * cdf).astype(BF)
            hid[r, lanes] = unit
            hid_f[r, lanes] = unit * hidden_row(i, h).astype(BF)

    def backward(first, last):
        @pl.loop(first * bands, last * bands)
        def _(t):
            i, h, r, lanes = spans(t)
            dh = dot_t(cot[r, :], weight(2, h))
            dh = dh + dot_t(cot_f[r, :], weight(3, h)) * hidden_row(i, h)
            unit = (dh * slope[r, lanes]).astype(BF)
            dpre[r, lanes] = unit
            dpre_f[r, lanes] = unit * signs[i, 2:3, lanes].astype(BF)

    def weight_grad(m, left, right):
        @pl.loop(0, bands)
        def _(h):
            lhs = left[:, pl.ds(pl.multiple_of(h * band, band), band)]
            for n in range(width // nblk):
                cols = slice(n * nblk, (n + 1) * nblk)
                part[m, pl.ds(h * per_band, per_band), :, :, cols] = (
                    dot_0(lhs, right[:, cols]).astype(BF).reshape(per_band, SIDE, share, nblk)
                )

    def scatter_rings(m, base):
        along_y = lambda j, h: part.at[m, :, j, rows_of(h)]
        along_x = lambda j, h: part.at[m, j, :, rows_of(h)]
        one = lambda j, h: part.at[m, j, y, rows_of(h)]
        two = lambda j, h: part.at[m, x, j, rows_of(h)]
        if m % 2 == 0:
            return Ring(at, "y", along_y, rs_s, rs_r, base), Ring(at, "x", one, rs_s, rs_r, base + 6)
        return Ring(at, "x", along_x, rs_s, rs_r, base), Ring(at, "y", two, rs_s, rs_r, base + 6)

    rs = [scatter_rings(m, 12 * m) for m in range(4)]

    def start1(m):
        rs[m][0].scatter_start([near1.at[m, k] for k in range(2)], [once1.at[m, k] for k in range(4)])

    def start2(m):
        rs[m][1].scatter_start([near2.at[m, k] for k in range(2)], [once2.at[m, k] for k in range(4)])

    row_groups = min(nk, 2)
    lane_groups = nk // row_groups
    zr, zl = share // row_groups, width // lane_groups

    def spot(j):
        return (
            pl.ds(pl.multiple_of(lax.div(j, lane_groups) * zr, zr), zr),
            pl.ds(pl.multiple_of(lax.rem(j, lane_groups) * zl, zl), zl),
        )

    z_live = {}

    def z_copy(m, stage, d, step, src, dst):
        copy = pltpu.make_async_remote_copy(
            src_ref=src,
            dst_ref=dst,
            send_sem=z_s.at[m, stage, d - 1],
            recv_sem=z_r.at[m, stage, d - 1],
            device_id=(lax.rem(z + step * d, nz), c, x, y),
            device_id_type=MESH_ID,
        )
        copy.start()
        z_live[m, stage, d] = copy

    def z_start(m):
        for d in range(1, nk):
            r, l = spot(lax.rem(zk + d, nk))
            z_copy(m, 0, d, 2, part.at[m, x, y, r, l], zbuf.at[m, d - 1])

    def z_spread(m):
        r, l = spot(zk)
        acc = part[m, x, y, r, l].astype(F32)
        for d in range(1, nk):
            z_live[m, 0, d].wait_recv()
            acc = acc + zbuf[m, d - 1].astype(F32)
        total[m, c, zp, r, l] = acc.astype(BF)
        for d in range(1, nk):
            place = total.at[m, c, zp, r, l]
            z_copy(m, 1, d, 2, place, place)

    beside = (lax.rem(z + nz - 1 + 2 * zp, nz), c, x, y)
    last = {}

    def z_hand(m):
        for d in range(1, nk):
            z_live[m, 1, d].wait_recv()
        own = total.at[m, c, zp]
        last[m, 0] = send(own, own, beside)
        last[m, 1] = send(own, own, partner)

    sum_refs = (mean_in_ref, sigma_in_ref, mean_out_ref, sigma_out_ref)

    def flat_sum(m):
        flat = total[m].reshape(4 * share, width)
        return flat.T if m < 2 else flat

    def z_finish(m):
        last[m, 0].wait_recv()
        far = total.at[m, c, 1 - zp]
        last[m, 2] = send(far, far, partner)

    def project(left, left_f, t, sign, slots):
        m = 2 * t

        @pl.loop(0, width // nblk)
        def _(n):
            lanes = pl.ds(pl.multiple_of(n * nblk, nblk), nblk)
            plain = w_all[m, :, :, :, lanes].reshape(own_hidden, nblk)
            noisy = w_all[m + 1, :, :, :, lanes].reshape(own_hidden, nblk)
            for i in slots:
                r = slice(i * patches, (i + 1) * patches)
                out = dot_n(left[r, :], plain)
                out = out + dot_n(left_f[r, :], noisy) * signs[i, sign : sign + 1, lanes]
                if i:
                    theirs[t, i - 1, :, lanes] = out.astype(BF)
                else:
                    mine[t, :, lanes] = out

    def relay(t, to_far):
        to_far.wait_recv()

        @pl.loop(0, patches // chunk)
        def _(i):
            r = pl.ds(pl.multiple_of(i * chunk, chunk), chunk)
            both = theirs[t, 1, r, :].astype(F32) + arrived[t, 1, r, :].astype(F32)
            theirs[t, 1, r, :] = both.astype(BF)

        return send(theirs.at[t, 1], arrived.at[t, 2], mate)

    forward(0, 2)
    sign_2.wait_recv()
    norm_2.wait_recv()
    norm_3 = send(norm.at[slot_rows(2)], norm.at[slot_rows(3)], partner)
    flip(norm_f, norm, 2, 0)
    forward(2, 3)
    for m in (2, 3):
        ag[m][1].gather_forward()
    sign_3.wait_recv()
    norm_3.wait_recv()
    flip(norm_f, norm, 3, 0)
    forward(3, 4)
    cot_2[1].wait_recv()
    cot_3.append(send(half_slot(2, 1), half_slot(3, 1), partner))
    flip(cot_f, cot, 2, 1)
    for copy in cot_3:
        copy.wait_recv()
    weight_grad(2, hid, cot)
    start1(2)
    for m in (2, 3):
        ag[m][1].gather_finish()
    project(hid, hid_f, 1, 1, (2, 3))
    mixed_far = send(theirs.at[1, 2], arrived.at[1, 1], partner)
    flip(cot_f, cot, 3, 1)
    weight_grad(3, hid_f, cot_f)
    start1(3)
    mixed_2 = relay(1, mixed_far)
    backward(0, 4)
    rs[2][0].scatter_forward(add_into)
    weight_grad(0, dpre, norm)
    start1(0)
    rs[3][0].scatter_forward(add_into)
    weight_grad(1, dpre_f, norm_f)
    start1(1)
    project(dpre, dpre_f, 0, 0, (2, 3))
    back_far = send(theirs.at[0, 2], arrived.at[0, 1], partner)

    def finish1(m):
        rs[m][0].scatter_finish(add_into)
        start2(m)

    def forward1(m):
        rs[m][0].scatter_forward(add_into)

    def forward2(m):
        rs[m][1].scatter_forward(add_into)

    def finish2(m):
        rs[m][1].scatter_finish(add_into)
        z_start(m)

    def gathered(t, r):
        return mine[t, r, :] + arrived[t, 0, r, :].astype(F32) + arrived[t, 2, r, :].astype(F32)

    forward1(0)
    finish1(2)
    back_2 = relay(0, back_far)
    forward1(1)
    finish1(3)
    project(hid, hid_f, 1, 1, (0, 1))
    mixed_1 = send(theirs.at[1, 0], arrived.at[1, 0], partner)
    finish1(0)
    finish1(1)
    forward2(2)
    forward2(3)
    forward2(0)
    forward2(1)
    finish2(2)
    finish2(3)
    finish2(0)
    finish2(1)
    project(dpre, dpre_f, 0, 0, (0, 1))
    back_1 = send(theirs.at[0, 0], arrived.at[0, 0], partner)
    z_spread(2)
    z_spread(3)
    mixed_1.wait_recv()
    mixed_2.wait_recv()

    @pl.loop(0, patches // chunk)
    def _(i):
        r = pl.ds(pl.multiple_of(i * chunk, chunk), chunk)
        out_ref[r, :] = (resid[r, :].astype(F32) + gathered(1, r)).astype(BF)

    z_spread(0)
    z_spread(1)
    z_hand(2)
    z_hand(3)
    back_1.wait_recv()
    back_2.wait_recv()

    @pl.loop(0, patches // chunk)
    def _(i):
        r = pl.ds(pl.multiple_of(i * chunk, chunk), chunk)
        _, ahat, rstd = stats(r)
        g = gathered(0, r) * gain
        back = rstd * (
            g
            - jnp.mean(g, axis=-1, keepdims=True)
            - ahat * jnp.mean(g * ahat, axis=-1, keepdims=True)
        )
        grad_ref[r, :] = (cot_ref[r, :].astype(F32) + back).astype(BF)

    z_hand(0)
    z_hand(1)
    z_finish(2)
    z_finish(3)
    for m in (2, 3):
        last[m, 1].wait_recv()
        last[m, 2].wait_recv()
        sum_refs[m][...] = flat_sum(m)
    z_finish(0)
    z_finish(1)
    for m in (0, 1):
        last[m, 1].wait_recv()
        last[m, 2].wait_recv()
        sum_refs[m][...] = flat_sum(m)

    for first, second in ag + rs:
        first.drain()
        second.drain()
    for copy in [*z_live.values(), *sends]:
        copy.wait_send()


def layer(gain, flips, mats, images, nz):
    patches, width = images[0].shape
    cols = mats[0].shape[1]
    share = cols // 4
    count = flips[0].shape[0]
    half = share // 2
    hidden = SIDE * SIDE * share
    four = 4 * patches
    nk = nz // 2
    row_groups = min(nk, 2)
    zr, zl = share // row_groups, width // (nk // row_groups)
    vmem = pl.BlockSpec(memory_space=pltpu.VMEM)
    any_space = pl.BlockSpec(memory_space=pl.ANY)
    dma = pltpu.SemaphoreType.DMA
    scratch = [
        pltpu.VMEM((4, SIDE, SIDE, share, width), BF),
        pltpu.VMEM((SIDE, SIDE, 8, cols), F32),
        pltpu.VMEM((4, 8, max(width, 2 * hidden)), F32),
        pltpu.VMEM((4, 8, max(width, 2 * hidden)), F32),
        pltpu.VMEM((four, width), BF),
        pltpu.VMEM((four, width), BF),
        pltpu.VMEM((four, width), BF),
        pltpu.VMEM((four, width), BF),
        pltpu.VMEM((patches, width), BF),
        pltpu.VMEM((four, hidden), BF),
        pltpu.VMEM((four, hidden), BF),
        pltpu.VMEM((four, hidden), F32),
        pltpu.VMEM((four, hidden), BF),
        pltpu.VMEM((four, hidden), BF),
        pltpu.VMEM((2, patches, width), F32),
        pltpu.VMEM((2, 3, patches, width), BF),
        pltpu.VMEM((2, 3, patches, width), BF),
        pltpu.VMEM((4, SIDE, SIDE, share, width), BF),
        pltpu.VMEM((4, 2, SIDE, half, width), BF),
        pltpu.VMEM((4, 4, SIDE, half, width), BF),
        pltpu.VMEM((4, 2, half, width), BF),
        pltpu.VMEM((4, 4, half, width), BF),
        pltpu.VMEM((4, nk - 1, zr, zl), BF),
        pltpu.VMEM((4, 2, 2, share, width), BF),
        dma((48,)),
        dma((48,)),
        dma((48,)),
        dma((48,)),
        dma((4, 2, nk - 1)),
        dma((4, 2, nk - 1)),
        dma((44,)),
        dma((44,)),
        dma((11,)),
        pltpu.VMEM((3, width, cols), BF),
        pltpu.VMEM((3, cols, width), BF),
        pltpu.VMEM((4, patches, width), BF),
        pltpu.VMEM((3, cols, width), BF),
        pltpu.VMEM((count, 8, cols), F32),
    ]
    return pl.pallas_call(
        functools.partial(kernel, nz),
        out_shape=(
            jax.ShapeDtypeStruct((patches, width), BF),
            jax.ShapeDtypeStruct((patches, width), BF),
            jax.ShapeDtypeStruct((width, cols), BF),
            jax.ShapeDtypeStruct((width, cols), BF),
            jax.ShapeDtypeStruct((cols, width), BF),
            jax.ShapeDtypeStruct((cols, width), BF),
        ),
        in_specs=[vmem] * 5 + [any_space] * 11,
        out_specs=(vmem,) * 6,
        scratch_shapes=scratch,
        compiler_params=pltpu.CompilerParams(
            collective_id=0, has_side_effects=True, vmem_limit_bytes=62 * 1024 * 1024
        ),
        name="layer",
    )(gain, *flips, *mats, *images)


def body(
    tokens,
    queries,
    keys,
    values,
    ln_gain,
    mean_in,
    sigma_in,
    noise_in,
    mean_out,
    sigma_out,
    noise_out,
    flip_in,
    flip_mid,
    flip_hidden,
    flip_out,
    cotangent,
):
    nz = lax.axis_size("z")
    out, grad, *sums = layer(
        ln_gain,
        (flip_in, flip_out, flip_mid, flip_hidden),
        (mean_in, sigma_in, noise_in, mean_out, sigma_out, noise_out),
        (queries[0], keys[0], values[0], tokens[0], cotangent[0]),
        nz,
    )
    grad_mean_in, grad_sigma_in, grad_mean_out, grad_sigma_out = (t.astype(F32) for t in sums)
    grad_sigma_in = grad_sigma_in * noise_in.astype(F32)
    grad_sigma_out = grad_sigma_out * noise_out.astype(F32)
    return out[None], grad[None], grad_mean_in, grad_sigma_in, grad_mean_out, grad_sigma_out


def solution(mesh):
    finer = Mesh(mesh.devices.reshape(-1, 2, SIDE, SIDE), ALL)
    images = P(ALL, None, None)
    cols = P(None, SEQ)
    rows = P(SEQ, None)
    in_specs = (
        images,
        images,
        images,
        images,
        P(),
        cols,
        cols,
        cols,
        rows,
        rows,
        rows,
        P(DP, None),
        P(DP, SEQ),
        P(DP, SEQ),
        P(DP, None),
        images,
    )
    out_specs = (images, images, cols, cols, rows, rows)
    return jax.shard_map(body, mesh=finer, in_specs=in_specs, out_specs=out_specs, check_vma=False)
```
